128 devices in a mesh: ep: 64 (over z, y, x), dp: 2 (over core).
Axes of the slice: x: 4, y: 4, z: 4, core: 2. Of those that a mesh axis runs over, the one named last changes fastest.
Arguments:
- tokens: bfloat16 [32768, 448], P(('dp', 'ep'))
- d_out: bfloat16 [32768, 448], P(('dp', 'ep'))
- expert_ids: int32 [2, 32768, 8], P(None, ('dp', 'ep'))
- gate_vals: float32 [2, 32768, 8], P(None, ('dp', 'ep'))
- w_mix: bfloat16 [2, 448, 448], replicated
- w_gate: bfloat16 [2, 256, 448, 128], P(None, 'ep')
- w_up: bfloat16 [2, 256, 448, 128], P(None, 'ep')
- w_down: bfloat16 [2, 256, 128, 448], P(None, 'ep')
Outputs:
- output 1: bfloat16 [32768, 448], P(('dp', 'ep'))
- output 2: bfloat16 [32768, 448], P(('dp', 'ep'))
- output 3: bfloat16 [2, 448, 448], replicated
- output 4: bfloat16 [2, 256, 448, 128], P(None, 'ep')
- output 5: bfloat16 [2, 256, 448, 128], P(None, 'ep')
- output 6: bfloat16 [2, 256, 128, 448], P(None, 'ep')
All inputs are finite; a program needn't handle non-finite values.
Results may differ from the reference program's by a relative error of at most 0.02.
Values are sent between devices in bfloat16 or wider.
A program may use at most 1 GiB of HBM per device.

```python
import jax
import jax.numpy as jnp

D = 448
FF = 128
EXPERTS = 256
TOP = 8
TOK = 256
NDEV = 128
LAYERS = 2
CAP = 24
HOT = 32

N_TOK = TOK * NDEV
CAP_ALL = CAP * NDEV


def route_device(hot_mask, dev_key):
    key_rest, key_run, key_tok = jax.random.split(dev_key, 3)
    rest_copies = TOK * TOP - HOT * CAP
    base_count = rest_copies // (EXPERTS - HOT)
    extra_count = rest_copies % (EXPERTS - HOT)
    shuffled = jax.random.permutation(key_rest, EXPERTS)
    cold_sorted = 1 - hot_mask[shuffled]
    cold_rank = jnp.cumsum(cold_sorted) - 1
    bonus_sorted = cold_sorted * (cold_rank < extra_count).astype(jnp.int32)
    bonus = jnp.zeros((EXPERTS,), jnp.int32).at[shuffled].set(bonus_sorted)
    counts = jnp.where(hot_mask == 1, CAP, base_count + bonus)
    run_order = jax.random.permutation(key_run, EXPERTS)
    flat_ids = jnp.repeat(run_order, counts[run_order], total_repeat_length=TOK * TOP)
    table = flat_ids.reshape(TOP, TOK).T
    return table[jax.random.permutation(key_tok, TOK)]


def route_layer(layer_key):
    key_hot, key_dev = jax.random.split(layer_key)
    hot_ids = jax.random.permutation(key_hot, EXPERTS)[:HOT]
    hot_mask = jnp.zeros((EXPERTS,), jnp.int32).at[hot_ids].set(1)
    per_device = jax.vmap(route_device, in_axes=(None, 0))(hot_mask, jax.random.split(key_dev, NDEV))
    return per_device.reshape(N_TOK, TOP)


def setup_inputs(seed: int = 0) -> dict:
    keys = jax.random.split(jax.random.key(seed), 8)
    tokens = jax.random.normal(keys[0], (N_TOK, D), jnp.float32).astype(jnp.bfloat16)
    d_out = jax.random.normal(keys[1], (N_TOK, D), jnp.float32).astype(jnp.bfloat16)
    expert_ids = jax.vmap(route_layer)(jax.random.split(keys[2], LAYERS))
    gate_vals = jax.random.uniform(keys[3], (LAYERS, N_TOK, TOP), jnp.float32, 0.5, 1.5) * TOP ** -0.5
    w_mix = (jax.random.normal(keys[4], (LAYERS, D, D), jnp.float32) * D ** -0.5).astype(jnp.bfloat16)
    w_gate = (jax.random.normal(keys[5], (LAYERS, EXPERTS, D, FF), jnp.float32) * D ** -0.5).astype(jnp.bfloat16)
    w_up = (jax.random.normal(keys[6], (LAYERS, EXPERTS, D, FF), jnp.float32) * D ** -0.5).astype(jnp.bfloat16)
    w_down = (jax.random.normal(keys[7], (LAYERS, EXPERTS, FF, D), jnp.float32) * FF ** -0.5).astype(jnp.bfloat16)
    return {'tokens': tokens, 'd_out': d_out, 'expert_ids': expert_ids, 'gate_vals': gate_vals,
            'w_mix': w_mix, 'w_gate': w_gate, 'w_up': w_up, 'w_down': w_down}


def silu_parts(pre_gate):
    sig_val = jax.nn.sigmoid(pre_gate)
    return pre_gate * sig_val, sig_val * (1.0 + pre_gate * (1.0 - sig_val))


def copy_slots(expert_ids):
    flat_ids = expert_ids.reshape(-1)
    sort_order = jnp.argsort(flat_ids, stable=True)
    sorted_ids = flat_ids[sort_order]
    counts = jnp.bincount(flat_ids, length=EXPERTS)
    starts = jnp.cumsum(counts) - counts
    rows_sorted = sorted_ids * CAP_ALL + jnp.arange(flat_ids.shape[0]) - starts[sorted_ids]
    return jnp.zeros_like(flat_ids).at[sort_order].set(rows_sorted)


def layer_forward(x_in, expert_ids, gate_vals, w_mix, w_gate, w_up, w_down):
    mixed = x_in.astype(jnp.float32) + jnp.dot(x_in, w_mix, preferred_element_type=jnp.float32)
    u_act = mixed.astype(jnp.bfloat16)
    copy_rows = copy_slots(expert_ids)
    copy_tok = jnp.arange(N_TOK * TOP) // TOP
    expert_in = jnp.zeros((EXPERTS * CAP_ALL, D), jnp.bfloat16).at[copy_rows].set(u_act[copy_tok])
    expert_in = expert_in.reshape(EXPERTS, CAP_ALL, D)
    expert_f = expert_in.astype(jnp.float32)
    pre_gate = jnp.einsum('ecd,edf->ecf', expert_f, w_gate.astype(jnp.float32))
    pre_up = jnp.einsum('ecd,edf->ecf', expert_f, w_up.astype(jnp.float32))
    act, _ = silu_parts(pre_gate)
    hidden = (act * pre_up).astype(jnp.bfloat16)
    expert_out = jnp.einsum('ecf,efd->ecd', hidden.astype(jnp.float32), w_down.astype(jnp.float32)).astype(jnp.bfloat16)
    out_copy = expert_out.reshape(EXPERTS * CAP_ALL, D)[copy_rows].reshape(N_TOK, TOP, D)
    y_out = u_act.astype(jnp.float32) + jnp.sum(gate_vals[:, :, None] * out_copy.astype(jnp.float32), axis=1)
    return y_out.astype(jnp.bfloat16), (x_in, copy_rows, expert_in, pre_gate, pre_up, hidden)


def layer_backward(saved, d_y, gate_vals, w_mix, w_gate, w_up, w_down):
    x_in, copy_rows, expert_in, pre_gate, pre_up, hidden = saved
    g_dy = (gate_vals[:, :, None] * d_y.astype(jnp.float32)[:, None, :]).astype(jnp.bfloat16).reshape(N_TOK * TOP, D)
    d_buf = jnp.zeros((EXPERTS * CAP_ALL, D), jnp.bfloat16).at[copy_rows].set(g_dy).reshape(EXPERTS, CAP_ALL, D)
    d_buf_f = d_buf.astype(jnp.float32)
    d_hidden = jnp.einsum('ecd,efd->ecf', d_buf_f, w_down.astype(jnp.float32))
    act, act_slope = silu_parts(pre_gate)
    d_pre_gate = (d_hidden * pre_up * act_slope).astype(jnp.bfloat16).astype(jnp.float32)
    d_pre_up = (d_hidden * act).astype(jnp.bfloat16).astype(jnp.float32)
    d_expert_in = (jnp.einsum('ecf,edf->ecd', d_pre_gate, w_gate.astype(jnp.float32))
                   + jnp.einsum('ecf,edf->ecd', d_pre_up, w_up.astype(jnp.float32))).astype(jnp.bfloat16)
    expert_f = expert_in.astype(jnp.float32)
    g_gate = jnp.einsum('ecd,ecf->edf', expert_f, d_pre_gate).astype(jnp.bfloat16)
    g_up = jnp.einsum('ecd,ecf->edf', expert_f, d_pre_up).astype(jnp.bfloat16)
    g_down = jnp.einsum('ecf,ecd->efd', hidden.astype(jnp.float32), d_buf_f).astype(jnp.bfloat16)
    d_copy = d_expert_in.reshape(EXPERTS * CAP_ALL, D)[copy_rows].reshape(N_TOK, TOP, D)
    d_u = (d_y.astype(jnp.float32) + jnp.sum(gate_vals[:, :, None] * d_copy.astype(jnp.float32), axis=1)).astype(jnp.bfloat16)
    g_mix = jnp.dot(x_in.T, d_u, preferred_element_type=jnp.float32).astype(jnp.bfloat16)
    d_x = (d_u.astype(jnp.float32) + jnp.dot(d_u, w_mix.T, preferred_element_type=jnp.float32)).astype(jnp.bfloat16)
    return d_x, (g_mix, g_gate, g_up, g_down)


def reference(tokens, d_out, expert_ids, gate_vals, w_mix, w_gate, w_up, w_down):
    layer_in = tokens
    saved_all = []
    for layer in range(LAYERS):
        layer_in, saved = layer_forward(layer_in, expert_ids[layer], gate_vals[layer], w_mix[layer],
                                        w_gate[layer], w_up[layer], w_down[layer])
        saved_all.append(saved)
    d_y = d_out
    grads = []
    for layer in reversed(range(LAYERS)):
        d_y, grad_set = layer_backward(saved_all[layer], d_y, gate_vals[layer], w_mix[layer],
                                       w_gate[layer], w_up[layer], w_down[layer])
        grads.insert(0, grad_set)
    return (layer_in, d_y,
            jnp.stack([entry[0] for entry in grads]),
            jnp.stack([entry[1] for entry in grads]),
            jnp.stack([entry[2] for entry in grads]),
            jnp.stack([entry[3] for entry in grads]))
```

```python
import jax
import jax.numpy as jnp
from jax import lax
from jax.sharding import Mesh, PartitionSpec as P

CAP_FACTOR = 3
F32 = jnp.float32
BF16 = jnp.bfloat16


def silu_parts(pre_gate):
    sig_val = jax.nn.sigmoid(pre_gate)
    return pre_gate * sig_val, sig_val * (1.0 + pre_gate * (1.0 - sig_val))


def split3(val):
    hi = lax.reduce_precision(val, 8, 7)
    rest = val - hi
    mid = lax.reduce_precision(rest, 8, 7)
    lo = rest - mid
    return hi.astype(BF16), mid.astype(BF16), lo.astype(BF16)


def dot(spec, a, b):
    return jnp.einsum(spec, a, b, preferred_element_type=F32)


def routing(ids, gates, my_experts, capacity):
    hit = ids[:, :, :, None] == my_experts[None, None, None, :]
    used = jnp.any(hit, axis=2)
    gate_te = jnp.sum(jnp.where(hit, gates[:, :, :, None], 0.0), axis=2)
    n_tok = ids.shape[1]
    row = lax.broadcasted_iota(jnp.int32, (n_tok, n_tok), 0)
    col = lax.broadcasted_iota(jnp.int32, (n_tok, n_tok), 1)
    lower = (col < row).astype(BF16)
    pos = dot('tu,sui->sti', lower, used.astype(BF16))
    pos = jnp.where(used, pos, -1.0)
    return pos, gate_te


def solution(mesh):
    m4 = Mesh(mesh.devices.reshape(4, 4, 4, 2), ('z', 'y', 'x', 'dp'))
    ep = ('z', 'y', 'x')
    tok_spec = P(('dp',) + ep, None)
    route_spec = P(None, ('dp',) + ep, None)
    whole_spec = P(None, None, None)
    expert_spec = P(None, ep, None, None)

    def device_step(tokens, d_out, expert_ids, gate_vals, w_mix, w_gate, w_up, w_down):
        n_layers = w_mix.shape[0]
        n_chip = w_gate.shape[1]
        n_half = n_chip // 2
        n_experts = n_chip * 64
        tok_local, d_model = tokens.shape
        ff = w_gate.shape[3]
        top_k = expert_ids.shape[2]
        capacity = (CAP_FACTOR * tok_local * top_k + n_experts - 1) // n_experts
        dp = lax.axis_index('dp')
        zi = lax.axis_index('z')
        n_mine = 16 * n_half
        loc = jnp.arange(n_mine, dtype=jnp.int32)
        my_experts = (zi * 16 + loc // n_half) * n_chip + dp * n_half + loc % n_half

        def gather_tokens(val):
            return lax.all_gather(val, ('z', 'dp'), axis=0, tiled=False).reshape(8, tok_local, -1)

        def scatter_tokens(part):
            return lax.psum_scatter(part.reshape(8 * tok_local, d_model), ('z', 'dp'),
                                    scatter_dimension=0, tiled=True)

        def gather_weights(layer):
            wg = lax.dynamic_slice_in_dim(w_gate[layer], dp * n_half, n_half, 0)
            wu = lax.dynamic_slice_in_dim(w_up[layer], dp * n_half, n_half, 0)
            wd = lax.dynamic_slice_in_dim(w_down[layer], dp * n_half, n_half, 0)
            pack = jnp.stack([wg, wu, jnp.swapaxes(wd, 1, 2)], axis=0)
            pack = pack.reshape(3 * n_half * d_model, ff)
            full = lax.all_gather(pack, ('y', 'x'), axis=0, tiled=False)
            full = full.reshape(16, 3, n_half, d_model, ff)
            return tuple(full[:, k].reshape(n_mine, d_model, ff) for k in range(3))

        def scatter_grads(gg, gu, gd):
            pack = jnp.stack([g.reshape(16, n_half, d_model, ff) for g in (gg, gu, gd)], axis=1)
            part = lax.psum_scatter(pack.reshape(16 * 3 * n_half * d_model, ff), ('y', 'x'),
                                    scatter_dimension=0, tiled=True)
            other = lax.ppermute(part, 'dp', [(0, 1), (1, 0)])
            lo = jnp.where(dp == 0, part, other).reshape(3, n_half, d_model, ff)
            hi = jnp.where(dp == 0, other, part).reshape(3, n_half, d_model, ff)
            both = jnp.concatenate([lo, hi], axis=1)
            return both[0], both[1], jnp.swapaxes(both[2], 1, 2)

        route_pack = []
        for layer in range(n_layers):
            route_pack.append(expert_ids[layer].astype(BF16))
            route_pack.extend(split3(gate_vals[layer]))
        route_pack = jnp.concatenate(route_pack, axis=1)

        slot_no = lax.broadcasted_iota(F32, (1, 1, capacity, 1), 2)

        weights = [gather_weights(layer) for layer in range(n_layers)]
        layer_in = tokens
        saved = []
        routes = None
        for layer in range(n_layers):
            u_act = (layer_in.astype(F32) + dot('td,de->te', layer_in, w_mix[layer])).astype(BF16)
            if layer == 0:
                got = gather_tokens(jnp.concatenate([u_act, route_pack], axis=1))
                u_all = got[:, :, :d_model]
                r_all = got[:, :, d_model:]
                routes = []
                for other in range(n_layers):
                    seg = r_all[:, :, other * 4 * top_k:(other + 1) * 4 * top_k]
                    ids = seg[:, :, :top_k].astype(jnp.int32)
                    gates = (seg[:, :, top_k:2 * top_k].astype(F32) + seg[:, :, 2 * top_k:3 * top_k].astype(F32)
                             + seg[:, :, 3 * top_k:].astype(F32))
                    routes.append(routing(ids, gates, my_experts, capacity))
            else:
                u_all = gather_tokens(u_act)
            pos, gate_te = routes[layer]
            pos_t = jnp.swapaxes(pos, 1, 2)
            sel = (pos_t[:, :, None, :] == slot_no)
            sel_b = sel.astype(BF16).reshape(8, n_mine * capacity, tok_local)
            gate_slot = jnp.sum(jnp.where(sel, jnp.swapaxes(gate_te, 1, 2)[:, :, None, :], 0.0), axis=3)
            comb = []
            for part in split3(gate_te):
                wide = jnp.where(pos[:, :, :, None] == slot_no.reshape(1, 1, 1, capacity),
                                 part[:, :, :, None], jnp.zeros((), BF16))
                comb.append(wide.reshape(8, tok_local, n_mine * capacity))

            def combine(rows, comb=comb):
                rows = rows.reshape(8, n_mine * capacity, d_model)
                total = dot('stk,skd->std', comb[2], rows)
                total = total + dot('stk,skd->std', comb[1], rows)
                return total + dot('stk,skd->std', comb[0], rows)

            wg, wu, wd = weights[layer]
            recv = dot('skt,std->skd', sel_b, u_all).astype(BF16).reshape(8, n_mine, capacity, d_model)
            pre_gate = dot('secd,edf->secf', recv, wg)
            pre_up = dot('secd,edf->secf', recv, wu)
            act, _ = silu_parts(pre_gate)
            hidden = (act * pre_up).astype(BF16)
            out = dot('secf,edf->secd', hidden, wd).astype(BF16)
            y_out = (u_act.astype(F32) + scatter_tokens(combine(out))).astype(BF16)
            saved.append((layer_in, recv, pre_gate, pre_up, hidden, sel_b, gate_slot, combine))
            layer_in = y_out

        d_y = d_out
        grads = []
        for layer in reversed(range(n_layers)):
            x_in, recv, pre_gate, pre_up, hidden, sel_b, gate_slot, combine = saved[layer]
            wg, wu, wd = weights[layer]
            dy_all = gather_tokens(d_y)
            dy_rows = dot('skt,std->skd', sel_b, dy_all).reshape(8, n_mine, capacity, d_model)
            grad_in = (gate_slot[..., None] * dy_rows).astype(BF16)
            d_hidden = dot('secd,edf->secf', grad_in, wd)
            act, act_slope = silu_parts(pre_gate)
            d_gate = (d_hidden * pre_up * act_slope).astype(BF16)
            d_up = (d_hidden * act).astype(BF16)
            d_recv = (dot('secf,edf->secd', d_gate, wg) + dot('secf,edf->secd', d_up, wu)).astype(BF16)
            gg = dot('secd,secf->edf', recv, d_gate).astype(BF16)
            gu = dot('secd,secf->edf', recv, d_up).astype(BF16)
            gd = dot('secd,secf->edf', grad_in, hidden).astype(BF16)
            d_u = (d_y.astype(F32) + scatter_tokens(combine(d_recv))).astype(BF16)
            g_mix = dot('td,te->de', x_in, d_u).astype(BF16)
            g_mix = lax.psum(g_mix, ('dp',) + ep)
            d_y = (d_u.astype(F32) + dot('te,de->td', d_u, w_mix[layer])).astype(BF16)
            grads.insert(0, (g_mix,) + scatter_grads(gg, gu, gd))
        return (layer_in, d_y) + tuple(jnp.stack([g[k] for g in grads]) for k in range(4))

    return jax.shard_map(device_step, mesh=m4,
                         in_specs=(tok_spec, tok_spec, route_spec, route_spec, whole_spec,
                                   expert_spec, expert_spec, expert_spec),
                         out_specs=(tok_spec, tok_spec, whole_spec, expert_spec, expert_spec, expert_spec),
                         check_vma=False)
```

```python
import functools
import jax
import jax.numpy as jnp
from jax import lax
from jax.experimental import pallas as pl
from jax.experimental.pallas import tpu as pltpu
from jax.sharding import Mesh, PartitionSpec as P

CAP_FACTOR = 3

F32 = jnp.float32
BF16 = jnp.bfloat16
MESH = pl.DeviceIdType.MESH
VMEM = pl.BlockSpec(memory_space=pltpu.VMEM)
COST = pl.CostEstimate(flops=8 * 10**9, bytes_accessed=10**7, transcendentals=0)


def enter(peers):
    barrier = pltpu.get_barrier_semaphore()
    for peer in peers:
        pl.semaphore_signal(barrier, inc=1, device_id=peer, device_id_type=MESH)
    pl.semaphore_wait(barrier, len(peers))


def send(src, dst, send_sems, recv_sems, index, peer):
    copy = pltpu.make_async_remote_copy(src_ref=src, dst_ref=dst, send_sem=send_sems.at[index],
                                        recv_sem=recv_sems.at[index], device_id=peer, device_id_type=MESH)
    copy.start()
    return copy


def line_peers():
    z, dp = lax.axis_index('z'), lax.axis_index('dp')
    up, down = {'z': lax.rem(z + 1, 4)}, {'z': lax.rem(z + 3, 4)}
    return z, dp, up, down, {'dp': 1 - dp}


N_AG = 9


def line_gather(src, dst, send_sems, recv_sems, base):
    z, dp, up, down, mate = line_peers()
    rows = src.shape[0]
    half = rows // 2
    me = z * 2 + dp
    below, above = lax.rem(z + 3, 4) * 2 + dp, lax.rem(z + 1, 4) * 2 + dp
    far = lax.rem(z + 2, 4) * 2 + dp
    lo, hi = pl.ds(0, half), pl.ds(half, half)
    go = functools.partial(send, send_sems=send_sems, recv_sems=recv_sems)
    to_up = go(src, dst.at[me], index=base, peer=up)
    to_down = go(src, dst.at[me], index=base + 1, peer=down)
    to_mate = go(src, dst.at[me], index=base + 2, peer=mate)
    dst[me] = src[...]
    to_up.wait_recv()
    relay_up = go(dst.at[below, lo], dst.at[below, lo], index=base + 3, peer=up)
    mate_below = go(dst.at[below], dst.at[below], index=base + 5, peer=mate)
    to_down.wait_recv()
    relay_down = go(dst.at[above, hi], dst.at[above, hi], index=base + 4, peer=down)
    mate_above = go(dst.at[above], dst.at[above], index=base + 6, peer=mate)
    relay_up.wait_recv()
    mate_lo = go(dst.at[far, lo], dst.at[far, lo], index=base + 7, peer=mate)
    relay_down.wait_recv()
    mate_hi = go(dst.at[far, hi], dst.at[far, hi], index=base + 8, peer=mate)
    for copy in (to_mate, mate_below, mate_above, mate_lo, mate_hi):
        copy.wait_recv()
    for copy in (to_up, to_down, to_mate, relay_up, relay_down, mate_below, mate_above, mate_lo, mate_hi):
        copy.wait_send()


N_RS = 10


def line_reduce(part, d_part, sums, relay_lo, relay_hi, in_lo, in_hi, send_sems, recv_sems, base):
    z, dp, up, down, mate = line_peers()
    half = part.shape[1] // 2
    lo, hi = pl.ds(0, half), pl.ds(half, half)
    order = [lax.rem(z + 2, 4), lax.rem(z + 1, 4), lax.rem(z + 3, 4), z]
    go = functools.partial(send, send_sems=send_sems, recv_sems=recv_sems)
    swaps = [go(part.at[zk * 2 + 1 - dp], d_part.at[k], index=base + k, peer=mate) for k, zk in enumerate(order)]
    swaps[0].wait_recv()
    sums[0] = part[order[0] * 2 + dp] + d_part[0]
    far_up = go(sums.at[0, lo], relay_lo, index=base + 4, peer=up)
    far_down = go(sums.at[0, hi], relay_hi, index=base + 5, peer=down)
    swaps[1].wait_recv()
    sums[1] = part[order[1] * 2 + dp] + d_part[1]
    up_hi = go(sums.at[1, hi], in_lo.at[hi], index=base + 6, peer=up)
    swaps[2].wait_recv()
    sums[2] = part[order[2] * 2 + dp] + d_part[2]
    down_lo = go(sums.at[2, lo], in_hi.at[lo], index=base + 7, peer=down)
    swaps[3].wait_recv()
    sums[3] = part[order[3] * 2 + dp] + d_part[3]
    far_up.wait_recv()
    sums[1, lo] = sums[1, lo] + relay_lo[...]
    up_lo = go(sums.at[1, lo], in_lo.at[lo], index=base + 8, peer=up)
    far_down.wait_recv()
    sums[2, hi] = sums[2, hi] + relay_hi[...]
    down_hi = go(sums.at[2, hi], in_hi.at[hi], index=base + 9, peer=down)
    up_hi.wait_recv()
    down_lo.wait_recv()
    up_lo.wait_recv()
    down_hi.wait_recv()
    for copy in swaps + [far_up, far_down, up_hi, down_lo, up_lo, down_hi]:
        copy.wait_send()
    return sums[3] + in_lo[...] + in_hi[...]


def reduce_scratch(tok, width):
    return [pltpu.VMEM((4, tok, width), F32), pltpu.VMEM((4, tok, width), F32),
            pltpu.VMEM((tok // 2, width), F32), pltpu.VMEM((tok // 2, width), F32),
            pltpu.VMEM((tok, width), F32), pltpu.VMEM((tok, width), F32)]


def params(collective_id):
    return pltpu.CompilerParams(collective_id=collective_id, has_side_effects=True,
                                vmem_limit_bytes=60 * 1024 * 1024)


def gather_kernel(src, dst, send_sems, recv_sems):
    _, _, up, down, mate = line_peers()
    enter((up, down, mate))
    line_gather(src, dst, send_sems, recv_sems, 0)


def gather_line(val, collective_id):
    return pl.pallas_call(
        gather_kernel, name='gather_line',
        out_shape=jax.ShapeDtypeStruct((8,) + val.shape, val.dtype),
        in_specs=[VMEM], out_specs=VMEM,
        scratch_shapes=[pltpu.SemaphoreType.DMA((N_AG,)), pltpu.SemaphoreType.DMA((N_AG,))],
        cost_estimate=COST, compiler_params=params(collective_id))(val)


def pass_kernel(transpose, want_all, part, base, w_mix, y_ref, next_ref, *rest):
    if want_all:
        all_ref, rest = rest[0], rest[1:]
    bufs, (send_sems, recv_sems) = rest[:-2], rest[-2:]
    _, _, up, down, mate = line_peers()
    enter((up, down, mate))
    total = line_reduce(part, *bufs, send_sems, recv_sems, 0)
    y_val = (base[...].astype(F32) + total).astype(BF16)
    y_ref[...] = y_val
    contract = (((1,), (1 if transpose else 0,)), ((), ()))
    mixed = lax.dot_general(y_val, w_mix[...], contract, preferred_element_type=F32)
    next_ref[...] = (y_val.astype(F32) + mixed).astype(BF16)
    if want_all:
        line_gather(next_ref, all_ref, send_sems, recv_sems, N_RS)


def pass_line(part, base, w_mix, transpose, want_all, collective_id):
    _, tok, width = part.shape
    block = jax.ShapeDtypeStruct((tok, width), BF16)
    outs = [block, block] + ([jax.ShapeDtypeStruct((8, tok, width), BF16)] if want_all else [])
    n_sem = N_RS + (N_AG if want_all else 0)
    return pl.pallas_call(
        functools.partial(pass_kernel, transpose, want_all), name='pass_line',
        out_shape=outs, in_specs=[VMEM] * 3, out_specs=[VMEM] * len(outs),
        scratch_shapes=reduce_scratch(tok, width) + [pltpu.SemaphoreType.DMA((n_sem,)),
                                                     pltpu.SemaphoreType.DMA((n_sem,))],
        cost_estimate=COST, compiler_params=params(collective_id))(part, base, w_mix)


def finish_kernel(part, base, y_ref, *rest):
    bufs, (send_sems, recv_sems) = rest[:-2], rest[-2:]
    _, _, up, down, mate = line_peers()
    enter((up, down, mate))
    total = line_reduce(part, *bufs, send_sems, recv_sems, 0)
    y_ref[...] = (base[...].astype(F32) + total).astype(BF16)


def finish_line(part, base, collective_id):
    _, tok, width = part.shape
    return pl.pallas_call(
        finish_kernel, name='finish_line',
        out_shape=jax.ShapeDtypeStruct((tok, width), BF16), in_specs=[VMEM] * 2, out_specs=VMEM,
        scratch_shapes=reduce_scratch(tok, width) + [pltpu.SemaphoreType.DMA((N_RS,)),
                                                     pltpu.SemaphoreType.DMA((N_RS,))],
        cost_estimate=COST, compiler_params=params(collective_id))(part, base)


def mix_kernel(grad, out, mate_in, quarter_in, block, y_in, y_out, z_in, z_out, send_sems, recv_sems):
    dp = lax.axis_index('dp')
    mate = {'dp': 1 - dp}
    at = {axis: lax.axis_index(axis) for axis in 'xyz'}
    peers = {axis: [{axis: lax.rem(at[axis] + k, 4)} for k in (1, 2, 3)] for axis in 'xyz'}
    enter(peers['x'] + peers['y'] + peers['z'] + [mate])
    quarter = grad.shape[1] // 4
    go = functools.partial(send, send_sems=send_sems, recv_sems=recv_sems)
    copies = []
    swap = go(grad.at[1 - dp], mate_in, index=0, peer=mate)
    swap.wait_recv()
    block[...] = (grad[dp].astype(F32) + mate_in[...].astype(F32)).astype(BF16)
    mine = pl.ds(pl.multiple_of(at['x'] * quarter, quarter), quarter)
    stage = []
    for k in range(3):
        rows = pl.ds(pl.multiple_of(lax.rem(at['x'] + k + 1, 4) * quarter, quarter), quarter)
        stage.append(go(block.at[rows], quarter_in.at[k], index=1 + k, peer=peers['x'][k]))
    copies += [swap] + stage
    total = block[mine].astype(F32)
    for k in range(3):
        stage[k].wait_recv()
        total = total + quarter_in[k].astype(F32)
    for axis, buf_in, buf_out, base in (('y', y_in, y_out, 4), ('z', z_in, z_out, 7)):
        buf_out[...] = total.astype(BF16)
        stage = [go(buf_out, buf_in.at[k], index=base + k, peer=peers[axis][k]) for k in range(3)]
        copies += stage
        terms = [buf_out[...].astype(F32)]
        for k in range(3):
            stage[k].wait_recv()
            terms.append(buf_in[k].astype(F32))
        here = at[axis]
        total = None
        for coord in range(4):
            term = jnp.zeros_like(terms[0])
            for k in range(4):
                source = lax.rem(here + 4 - k, 4)
                term = jnp.where(source == coord, terms[k], term)
            total = term if total is None else total + term
    final = total.astype(BF16)
    out[dp, mine] = final
    stage = [go(out.at[dp, mine], out.at[dp, mine], index=10 + k, peer=peers['x'][k]) for k in range(3)]
    copies += stage
    for k in range(3):
        stage[k].wait_recv()
    swap = go(out.at[dp], out.at[dp], index=13, peer=mate)
    swap.wait_recv()
    copies.append(swap)
    for copy in copies:
        copy.wait_send()


def mix_sum(grad, collective_id):
    n_layers, rows, width = grad.shape
    quarter = rows // 4
    return pl.pallas_call(
        mix_kernel, name='mix_sum',
        out_shape=jax.ShapeDtypeStruct(grad.shape, BF16), in_specs=[VMEM], out_specs=VMEM,
        scratch_shapes=[pltpu.VMEM((rows, width), BF16), pltpu.VMEM((3, quarter, width), BF16),
                        pltpu.VMEM((rows, width), BF16),
                        pltpu.VMEM((3, quarter, width), BF16), pltpu.VMEM((quarter, width), BF16),
                        pltpu.VMEM((3, quarter, width), BF16), pltpu.VMEM((quarter, width), BF16),
                        pltpu.SemaphoreType.DMA((14,)), pltpu.SemaphoreType.DMA((14,))],
        cost_estimate=COST, compiler_params=params(collective_id))(grad)


def silu_parts(pre_gate):
    sig_val = jax.nn.sigmoid(pre_gate)
    return pre_gate * sig_val, sig_val * (1.0 + pre_gate * (1.0 - sig_val))


def split3(val):
    hi = lax.reduce_precision(val, 8, 7)
    rest = val - hi
    mid = lax.reduce_precision(rest, 8, 7)
    lo = rest - mid
    return hi.astype(BF16), mid.astype(BF16), lo.astype(BF16)


def dot(spec, a, b):
    return jnp.einsum(spec, a, b, preferred_element_type=F32)


def routing(ids, gates, my_experts, capacity):
    hit = ids[:, :, :, None] == my_experts[None, None, None, :]
    used = jnp.any(hit, axis=2)
    gate_te = jnp.sum(jnp.where(hit, gates[:, :, :, None], 0.0), axis=2)
    n_tok = ids.shape[1]
    row = lax.broadcasted_iota(jnp.int32, (n_tok, n_tok), 0)
    col = lax.broadcasted_iota(jnp.int32, (n_tok, n_tok), 1)
    lower = (col < row).astype(BF16)
    pos = dot('tu,sui->sti', lower, used.astype(BF16))
    pos = jnp.where(used, pos, -1.0)
    return pos, gate_te


def solution(mesh):
    m4 = Mesh(mesh.devices.reshape(4, 4, 4, 2), ('z', 'y', 'x', 'dp'))
    ep = ('z', 'y', 'x')
    tok_spec = P(('dp',) + ep, None)
    route_spec = P(None, ('dp',) + ep, None)
    whole_spec = P(None, None, None)
    expert_spec = P(None, ep, None, None)

    def device_step(tokens, d_out, expert_ids, gate_vals, w_mix, w_gate, w_up, w_down):
        n_layers = w_mix.shape[0]
        n_chip = w_gate.shape[1]
        n_half = n_chip // 2
        n_experts = n_chip * 64
        tok_local, d_model = tokens.shape
        ff = w_gate.shape[3]
        top_k = expert_ids.shape[2]
        capacity = (CAP_FACTOR * tok_local * top_k + n_experts - 1) // n_experts
        dp = lax.axis_index('dp')
        zi = lax.axis_index('z')
        n_mine = 16 * n_half
        loc = jnp.arange(n_mine, dtype=jnp.int32)
        my_experts = (zi * 16 + loc // n_half) * n_chip + dp * n_half + loc % n_half

        def gather_weights(layer):
            wg = lax.dynamic_slice_in_dim(w_gate[layer], dp * n_half, n_half, 0)
            wu = lax.dynamic_slice_in_dim(w_up[layer], dp * n_half, n_half, 0)
            wd = lax.dynamic_slice_in_dim(w_down[layer], dp * n_half, n_half, 0)
            pack = jnp.stack([wg, wu, jnp.swapaxes(wd, 1, 2)], axis=0)
            pack = pack.reshape(3 * n_half * d_model, ff)
            full = lax.all_gather(pack, ('y', 'x'), axis=0, tiled=False)
            full = full.reshape(16, 3, n_half, d_model, ff)
            return tuple(full[:, k].reshape(n_mine, d_model, ff) for k in range(3))

        def pack_grads(gg, gu, gd):
            pack = jnp.stack([g.reshape(16, n_half, d_model, ff) for g in (gg, gu, gd)], axis=1)
            return pack.reshape(16 * 3 * n_half * d_model, ff)

        def scatter_grads(pack):
            part = lax.psum_scatter(pack, ('y', 'x'),
                                    scatter_dimension=0, tiled=True)
            other = lax.ppermute(part, 'dp', [(0, 1), (1, 0)])
            lo = jnp.where(dp == 0, part, other).reshape(3, n_half, d_model, ff)
            hi = jnp.where(dp == 0, other, part).reshape(3, n_half, d_model, ff)
            both = jnp.concatenate([lo, hi], axis=1)
            return both[0], both[1], jnp.swapaxes(both[2], 1, 2)

        route_pack = []
        for layer in range(n_layers):
            route_pack.append(expert_ids[layer].astype(BF16))
            route_pack.extend(split3(gate_vals[layer]))
        route_pack = jnp.concatenate(route_pack, axis=1)

        slot_no = lax.broadcasted_iota(F32, (1, 1, capacity, 1), 2)

        weights = [gather_weights(layer) for layer in range(n_layers)]

        def expand(pos, gate_te):
            pos_t = jnp.swapaxes(pos, 1, 2)
            sel = (pos_t[:, :, None, :] == slot_no)
            sel_b = sel.astype(BF16).reshape(8, n_mine * capacity, tok_local)
            gate_slot = jnp.sum(jnp.where(sel, jnp.swapaxes(gate_te, 1, 2)[:, :, None, :], 0.0), axis=3)
            comb = []
            for part in split3(gate_te):
                wide = jnp.where(pos[:, :, :, None] == slot_no.reshape(1, 1, 1, capacity),
                                 part[:, :, :, None], jnp.zeros((), BF16))
                comb.append(wide.reshape(8, tok_local, n_mine * capacity))

            def combine(rows):
                rows = rows.reshape(8, n_mine * capacity, d_model)
                total = dot('stk,skd->std', comb[2], rows)
                total = total + dot('stk,skd->std', comb[1], rows)
                return total + dot('stk,skd->std', comb[0], rows)

            return sel_b, gate_slot, combine

        u_act = (tokens.astype(F32) + dot('td,de->te', tokens, w_mix[0])).astype(BF16)
        pad = route_pack.shape[1]
        first = jnp.concatenate([jnp.concatenate([u_act, route_pack], axis=1),
                                 jnp.pad(d_out, ((0, 0), (0, pad)))], axis=0)
        got = gather_line(first, 1)
        u_all = got[:, :tok_local, :d_model]
        dy_all = got[:, tok_local:, :d_model]
        r_all = got[:, :tok_local, d_model:]
        routes = []
        for layer in range(n_layers):
            seg = r_all[:, :, layer * 4 * top_k:(layer + 1) * 4 * top_k]
            ids = seg[:, :, :top_k].astype(jnp.int32)
            gates = (seg[:, :, top_k:2 * top_k].astype(F32) + seg[:, :, 2 * top_k:3 * top_k].astype(F32)
                     + seg[:, :, 3 * top_k:].astype(F32))
            routes.append(expand(*routing(ids, gates, my_experts, capacity)))

        layer_in = tokens
        saved = []
        for layer in range(n_layers):
            sel_b, gate_slot, combine = routes[layer]
            wg, wu, wd = weights[layer]
            recv = dot('skt,std->skd', sel_b, u_all).astype(BF16).reshape(8, n_mine, capacity, d_model)
            pre_gate = dot('secd,edf->secf', recv, wg)
            pre_up = dot('secd,edf->secf', recv, wu)
            act, _ = silu_parts(pre_gate)
            hidden = (act * pre_up).astype(BF16)
            saved.append((layer_in, u_act, recv, pre_gate, pre_up, hidden))
            if layer < n_layers - 1:
                out = dot('secf,edf->secd', hidden, wd).astype(BF16)
                layer_in, u_act, u_all = pass_line(combine(out), u_act, w_mix[layer + 1], False, True, 2 + layer)

        d_y = d_out
        mix_grads = []
        grads = []
        for layer in reversed(range(n_layers)):
            x_in, u_act, recv, pre_gate, pre_up, hidden = saved[layer]
            sel_b, gate_slot, combine = routes[layer]
            wg, wu, wd = weights[layer]
            dy_rows = dot('skt,std->skd', sel_b, dy_all).reshape(8, n_mine, capacity, d_model)
            grad_in = (gate_slot[..., None] * dy_rows).astype(BF16)
            d_hidden = dot('secd,edf->secf', grad_in, wd)
            act, act_slope = silu_parts(pre_gate)
            d_gate = (d_hidden * pre_up * act_slope).astype(BF16)
            d_up = (d_hidden * act).astype(BF16)
            gg = dot('secd,secf->edf', recv, d_gate).astype(BF16)
            gu = dot('secd,secf->edf', recv, d_up).astype(BF16)
            gd = dot('secd,secf->edf', grad_in, hidden).astype(BF16)
            pack = pack_grads(gg, gu, gd)
            pack, d_gate, d_up, hidden = lax.optimization_barrier((pack, d_gate, d_up, hidden))
            grads.insert(0, scatter_grads(pack))
            d_recv = (dot('secf,edf->secd', d_gate, wg) + dot('secf,edf->secd', d_up, wu)).astype(BF16)
            part = combine(d_recv)
            if layer > 0:
                d_u, d_y, dy_all = pass_line(part, d_y, w_mix[layer], True, True, 4 + layer)
            else:
                d_u, d_y = pass_line(part, d_y, w_mix[layer], True, False, 4)
            mix_grads.insert(0, dot('td,te->de', x_in, d_u).astype(BF16))
            if layer == n_layers - 1:
                top = (hidden, u_act, combine, wd)
        hidden, u_act, combine, wd = top
        hidden, d_y = lax.optimization_barrier((hidden, d_y))
        out = dot('secf,edf->secd', hidden, wd).astype(BF16)
        layer_out = finish_line(combine(out), u_act, 6)
        mix_out = mix_sum(jnp.stack(mix_grads), 7)
        return (layer_out, d_y, mix_out) + tuple(jnp.stack([g[k] for g in grads]) for k in range(3))

    return jax.shard_map(device_step, mesh=m4,
                         in_specs=(tok_spec, tok_spec, route_spec, route_spec, whole_spec,
                                   expert_spec, expert_spec, expert_spec),
                         out_specs=(tok_spec, tok_spec, whole_spec, expert_spec, expert_spec, expert_spec),
                         check_vma=False)
```

```python
import functools
import jax
import jax.numpy as jnp
from jax import lax
from jax.experimental import pallas as pl
from jax.experimental.pallas import tpu as pltpu
from jax.sharding import Mesh, PartitionSpec as P


F32 = jnp.float32
BF16 = jnp.bfloat16
MESH = pl.DeviceIdType.MESH
VMEM = pl.BlockSpec(memory_space=pltpu.VMEM)
COST = pl.CostEstimate(flops=8 * 10**9, bytes_accessed=10**7, transcendentals=0)


def enter(peers):
    barrier = pltpu.get_barrier_semaphore()
    for peer in peers:
        pl.semaphore_signal(barrier, inc=1, device_id=peer, device_id_type=MESH)
    pl.semaphore_wait(barrier, len(peers))


def send(src, dst, send_sems, recv_sems, index, peer):
    copy = pltpu.make_async_remote_copy(src_ref=src, dst_ref=dst, send_sem=send_sems.at[index],
                                        recv_sem=recv_sems.at[index], device_id=peer, device_id_type=MESH)
    copy.start()
    return copy


def line_peers():
    z, dp = lax.axis_index('z'), lax.axis_index('dp')
    up, down = {'z': lax.rem(z + 1, 4)}, {'z': lax.rem(z + 3, 4)}
    return z, dp, up, down, {'dp': 1 - dp}


N_AG = 9


def line_gather(src, dst, send_sems, recv_sems, base):
    z, dp, up, down, mate = line_peers()
    rows = src.shape[0]
    half = rows // 2
    me = z * 2 + dp
    below, above = lax.rem(z + 3, 4) * 2 + dp, lax.rem(z + 1, 4) * 2 + dp
    far = lax.rem(z + 2, 4) * 2 + dp
    lo, hi = pl.ds(0, half), pl.ds(half, half)
    go = functools.partial(send, send_sems=send_sems, recv_sems=recv_sems)
    to_up = go(src, dst.at[me], index=base, peer=up)
    to_down = go(src, dst.at[me], index=base + 1, peer=down)
    to_mate = go(src, dst.at[me], index=base + 2, peer=mate)
    dst[me] = src[...]
    to_up.wait_recv()
    relay_up = go(dst.at[below, lo], dst.at[below, lo], index=base + 3, peer=up)
    mate_below = go(dst.at[below], dst.at[below], index=base + 5, peer=mate)
    to_down.wait_recv()
    relay_down = go(dst.at[above, hi], dst.at[above, hi], index=base + 4, peer=down)
    mate_above = go(dst.at[above], dst.at[above], index=base + 6, peer=mate)
    relay_up.wait_recv()
    mate_lo = go(dst.at[far, lo], dst.at[far, lo], index=base + 7, peer=mate)
    relay_down.wait_recv()
    mate_hi = go(dst.at[far, hi], dst.at[far, hi], index=base + 8, peer=mate)
    for copy in (to_mate, mate_below, mate_above, mate_lo, mate_hi):
        copy.wait_recv()
    for copy in (to_up, to_down, to_mate, relay_up, relay_down, mate_below, mate_above, mate_lo, mate_hi):
        copy.wait_send()


N_RS = 10


def line_reduce(part, d_part, sums, relay_lo, relay_hi, in_lo, in_hi, send_sems, recv_sems, base):
    z, dp, up, down, mate = line_peers()
    half = part.shape[1] // 2
    lo, hi = pl.ds(0, half), pl.ds(half, half)
    order = [lax.rem(z + 2, 4), lax.rem(z + 1, 4), lax.rem(z + 3, 4), z]
    go = functools.partial(send, send_sems=send_sems, recv_sems=recv_sems)
    swaps = [go(part.at[zk * 2 + 1 - dp], d_part.at[k], index=base + k, peer=mate) for k, zk in enumerate(order)]
    swaps[0].wait_recv()
    sums[0] = part[order[0] * 2 + dp] + d_part[0]
    far_up = go(sums.at[0, lo], relay_lo, index=base + 4, peer=up)
    far_down = go(sums.at[0, hi], relay_hi, index=base + 5, peer=down)
    swaps[1].wait_recv()
    sums[1] = part[order[1] * 2 + dp] + d_part[1]
    up_hi = go(sums.at[1, hi], in_lo.at[hi], index=base + 6, peer=up)
    swaps[2].wait_recv()
    sums[2] = part[order[2] * 2 + dp] + d_part[2]
    down_lo = go(sums.at[2, lo], in_hi.at[lo], index=base + 7, peer=down)
    swaps[3].wait_recv()
    sums[3] = part[order[3] * 2 + dp] + d_part[3]
    far_up.wait_recv()
    sums[1, lo] = sums[1, lo] + relay_lo[...]
    up_lo = go(sums.at[1, lo], in_lo.at[lo], index=base + 8, peer=up)
    far_down.wait_recv()
    sums[2, hi] = sums[2, hi] + relay_hi[...]
    down_hi = go(sums.at[2, hi], in_hi.at[hi], index=base + 9, peer=down)
    up_hi.wait_recv()
    down_lo.wait_recv()
    up_lo.wait_recv()
    down_hi.wait_recv()
    for copy in swaps + [far_up, far_down, up_hi, down_lo, up_lo, down_hi]:
        copy.wait_send()
    return sums[3] + in_lo[...] + in_hi[...]


def reduce_scratch(tok, width):
    return [pltpu.VMEM((4, tok, width), F32), pltpu.VMEM((4, tok, width), F32),
            pltpu.VMEM((tok // 2, width), F32), pltpu.VMEM((tok // 2, width), F32),
            pltpu.VMEM((tok, width), F32), pltpu.VMEM((tok, width), F32)]


def params(collective_id):
    return pltpu.CompilerParams(collective_id=collective_id, has_side_effects=True,
                                vmem_limit_bytes=60 * 1024 * 1024)


def gather_kernel(src, dst, send_sems, recv_sems):
    _, _, up, down, mate = line_peers()
    enter((up, down, mate))
    line_gather(src, dst, send_sems, recv_sems, 0)


def gather_line(val, collective_id):
    return pl.pallas_call(
        gather_kernel, name='gather_line',
        out_shape=jax.ShapeDtypeStruct((8,) + val.shape, val.dtype),
        in_specs=[VMEM], out_specs=VMEM,
        scratch_shapes=[pltpu.SemaphoreType.DMA((N_AG,)), pltpu.SemaphoreType.DMA((N_AG,))],
        compiler_params=params(collective_id))(val)


def pass_kernel(transpose, want_all, part, base, w_mix, y_ref, next_ref, *rest):
    if want_all:
        all_ref, rest = rest[0], rest[1:]
    bufs, (send_sems, recv_sems) = rest[:-2], rest[-2:]
    _, _, up, down, mate = line_peers()
    enter((up, down, mate))
    total = line_reduce(part, *bufs, send_sems, recv_sems, 0)
    y_val = (base[...].astype(F32) + total).astype(BF16)
    y_ref[...] = y_val
    contract = (((1,), (1 if transpose else 0,)), ((), ()))
    mixed = lax.dot_general(y_val, w_mix[...], contract, preferred_element_type=F32)
    next_ref[...] = (y_val.astype(F32) + mixed).astype(BF16)
    if want_all:
        line_gather(next_ref, all_ref, send_sems, recv_sems, N_RS)


def pass_line(part, base, w_mix, transpose, want_all, collective_id):
    _, tok, width = part.shape
    block = jax.ShapeDtypeStruct((tok, width), BF16)
    outs = [block, block] + ([jax.ShapeDtypeStruct((8, tok, width), BF16)] if want_all else [])
    n_sem = N_RS + (N_AG if want_all else 0)
    return pl.pallas_call(
        functools.partial(pass_kernel, transpose, want_all), name='pass_line',
        out_shape=outs, in_specs=[VMEM] * 3, out_specs=[VMEM] * len(outs),
        scratch_shapes=reduce_scratch(tok, width) + [pltpu.SemaphoreType.DMA((n_sem,)),
                                                     pltpu.SemaphoreType.DMA((n_sem,))],
        compiler_params=params(collective_id))(part, base, w_mix)


def finish_kernel(part, base, y_ref, *rest):
    bufs, (send_sems, recv_sems) = rest[:-2], rest[-2:]
    _, _, up, down, mate = line_peers()
    enter((up, down, mate))
    total = line_reduce(part, *bufs, send_sems, recv_sems, 0)
    y_ref[...] = (base[...].astype(F32) + total).astype(BF16)


def finish_line(part, base, collective_id):
    _, tok, width = part.shape
    return pl.pallas_call(
        finish_kernel, name='finish_line',
        out_shape=jax.ShapeDtypeStruct((tok, width), BF16), in_specs=[VMEM] * 2, out_specs=VMEM,
        scratch_shapes=reduce_scratch(tok, width) + [pltpu.SemaphoreType.DMA((N_RS,)),
                                                     pltpu.SemaphoreType.DMA((N_RS,))],
        compiler_params=params(collective_id))(part, base)


def mix_kernel(grad, out, mate_in, quarter_in, block, y_in, y_out, z_in, z_out, send_sems, recv_sems):
    dp = lax.axis_index('dp')
    mate = {'dp': 1 - dp}
    at = {axis: lax.axis_index(axis) for axis in 'xyz'}
    peers = {axis: [{axis: lax.rem(at[axis] + k, 4)} for k in (1, 2, 3)] for axis in 'xyz'}
    enter(peers['x'] + peers['y'] + peers['z'] + [mate])
    quarter = grad.shape[1] // 4
    go = functools.partial(send, send_sems=send_sems, recv_sems=recv_sems)
    copies = []
    swap = go(grad.at[1 - dp], mate_in, index=0, peer=mate)
    swap.wait_recv()
    block[...] = (grad[dp].astype(F32) + mate_in[...].astype(F32)).astype(BF16)
    mine = pl.ds(pl.multiple_of(at['x'] * quarter, quarter), quarter)
    stage = []
    for k in range(3):
        rows = pl.ds(pl.multiple_of(lax.rem(at['x'] + k + 1, 4) * quarter, quarter), quarter)
        stage.append(go(block.at[rows], quarter_in.at[k], index=1 + k, peer=peers['x'][k]))
    copies += [swap] + stage
    total = block[mine].astype(F32)
    for k in range(3):
        stage[k].wait_recv()
        total = total + quarter_in[k].astype(F32)
    for axis, buf_in, buf_out, base in (('y', y_in, y_out, 4), ('z', z_in, z_out, 7)):
        buf_out[...] = total.astype(BF16)
        stage = [go(buf_out, buf_in.at[k], index=base + k, peer=peers[axis][k]) for k in range(3)]
        copies += stage
        terms = [buf_out[...].astype(F32)]
        for k in range(3):
            stage[k].wait_recv()
            terms.append(buf_in[k].astype(F32))
        here = at[axis]
        total = None
        for coord in range(4):
            term = jnp.zeros_like(terms[0])
            for k in range(4):
                source = lax.rem(here + 4 - k, 4)
                term = jnp.where(source == coord, terms[k], term)
            total = term if total is None else total + term
    final = total.astype(BF16)
    out[dp, mine] = final
    stage = [go(out.at[dp, mine], out.at[dp, mine], index=10 + k, peer=peers['x'][k]) for k in range(3)]
    copies += stage
    for k in range(3):
        stage[k].wait_recv()
    swap = go(out.at[dp], out.at[dp], index=13, peer=mate)
    swap.wait_recv()
    copies.append(swap)
    for copy in copies:
        copy.wait_send()


def mix_sum(grad, collective_id):
    _, rows, width = grad.shape
    quarter = rows // 4
    return pl.pallas_call(
        mix_kernel, name='mix_sum',
        out_shape=jax.ShapeDtypeStruct(grad.shape, BF16), in_specs=[VMEM], out_specs=VMEM,
        scratch_shapes=[pltpu.VMEM((rows, width), BF16), pltpu.VMEM((3, quarter, width), BF16),
                        pltpu.VMEM((rows, width), BF16),
                        pltpu.VMEM((3, quarter, width), BF16), pltpu.VMEM((quarter, width), BF16),
                        pltpu.VMEM((3, quarter, width), BF16), pltpu.VMEM((quarter, width), BF16),
                        pltpu.SemaphoreType.DMA((14,)), pltpu.SemaphoreType.DMA((14,))],
        compiler_params=params(collective_id))(grad)


def silu_parts(pre_gate):
    sig_val = jax.nn.sigmoid(pre_gate)
    return pre_gate * sig_val, sig_val * (1.0 + pre_gate * (1.0 - sig_val))


def split3(val):
    hi = lax.reduce_precision(val, 8, 7)
    rest = val - hi
    mid = lax.reduce_precision(rest, 8, 7)
    return hi, mid, rest - mid


def dot(spec, a, b):
    return jnp.einsum(spec, a, b, preferred_element_type=F32)


CHUNK = 8
SLOT = 32


def pick(pos_row, slots):
    return jnp.broadcast_to(pos_row, slots.shape) == slots


def one_hot(pos, source, values=None):
    n_tok = pos.shape[2]
    slots = lax.broadcasted_iota(jnp.int32, (SLOT, n_tok), 0).astype(F32)
    blocks = []
    for e in range(CHUNK):
        mask = pick(pos[source, e:e + 1, :], slots)
        val = 1.0 if values is None else jnp.broadcast_to(values[source, e:e + 1, :], mask.shape)
        blocks.append(jnp.where(mask, val, 0.0))
    return jnp.concatenate(blocks, axis=0)


def nn(a, b):
    return lax.dot_general(a, b, (((1,), (0,)), ((), ())), preferred_element_type=F32)


def nt(a, b):
    return lax.dot_general(a, b, (((1,), (1,)), ((), ())), preferred_element_type=F32)


def tn(a, b):
    return lax.dot_general(a, b, (((0,), (0,)), ((), ())), preferred_element_type=F32)


def forward_kernel(pos, u_all, w_in, recv, pre_gate, pre_up, hidden):
    for s in range(8):
        rows = nn(one_hot(pos, s).astype(BF16), u_all[s]).astype(BF16)
        for e in range(CHUNK):
            recv[e, s * SLOT:(s + 1) * SLOT, :] = rows[e * SLOT:(e + 1) * SLOT]
    for e in range(CHUNK):
        w_both = jnp.concatenate([w_in[e // 2, 0, e % 2], w_in[e // 2, 1, e % 2]], axis=1)
        both = nn(recv[e], w_both)
        a, b = both[:, :128], both[:, 128:]
        act, _ = silu_parts(a)
        pre_gate[e] = a
        pre_up[e] = b
        hidden[e] = (act * b).astype(BF16)


def route_spec_of(n_tok):
    return pl.BlockSpec((8, CHUNK, n_tok), lambda i: (0, i, 0))


def local_params():
    return pltpu.CompilerParams(vmem_limit_bytes=60 * 1024 * 1024)


def expert_forward(pos, u_all, weights):
    _, n_mine, n_tok = pos.shape
    width = u_all.shape[2]
    ff = weights.shape[4]
    rows = 8 * SLOT
    per = lambda last: pl.BlockSpec((CHUNK, rows, last), lambda i: (i, 0, 0))
    return pl.pallas_call(
        forward_kernel, name='expert_forward', grid=(n_mine // CHUNK,),
        out_shape=[jax.ShapeDtypeStruct((n_mine, rows, width), BF16),
                   jax.ShapeDtypeStruct((n_mine, rows, ff), F32),
                   jax.ShapeDtypeStruct((n_mine, rows, ff), F32),
                   jax.ShapeDtypeStruct((n_mine, rows, ff), BF16)],
        in_specs=[route_spec_of(n_tok), pl.BlockSpec(u_all.shape, lambda i: (0, 0, 0)),
                  pl.BlockSpec((CHUNK // 2, 2, 2, width, ff), lambda i: (i, 0, 0, 0, 0))],
        out_specs=[per(width), per(ff), per(ff), per(ff)],
        compiler_params=local_params())(pos, u_all, weights)


def combine_kernel(n_left, pos, hi, mid, lo, *refs):
    lefts, w_out, part, rows = refs[:n_left], refs[n_left], refs[n_left + 1], refs[n_left + 2]
    for e in range(CHUNK):
        left = jnp.concatenate([ref[e] for ref in lefts], axis=1)
        right = jnp.concatenate([w_out[e // 2, k, e % 2] for k in range(n_left)], axis=1)
        rows[e] = nt(left, right).astype(BF16)
    for s in range(8):
        mine = jnp.concatenate([rows[e, s * SLOT:(s + 1) * SLOT, :] for e in range(CHUNK)], axis=0)
        val = tn(one_hot(pos, s, lo).astype(BF16), mine)
        val = val + tn(one_hot(pos, s, mid).astype(BF16), mine)
        val = val + tn(one_hot(pos, s, hi).astype(BF16), mine)

        @pl.when(pl.program_id(0) == 0)
        def _(val=val, s=s):
            part[s] = val

        @pl.when(pl.program_id(0) > 0)
        def _(val=val, s=s):
            part[s] = part[s] + val


def expert_combine(pos, gate_parts, lefts, weights, which):
    _, n_mine, n_tok = pos.shape
    width, ff = weights.shape[3:]
    rows = 8 * SLOT
    n_left = len(lefts)
    per = pl.BlockSpec((CHUNK, rows, ff), lambda i: (i, 0, 0))
    return pl.pallas_call(
        functools.partial(combine_kernel, n_left), name='expert_combine', grid=(n_mine // CHUNK,),
        out_shape=jax.ShapeDtypeStruct((8, n_tok, width), F32),
        in_specs=[route_spec_of(n_tok)] * 4 + [per] * n_left
        + [pl.BlockSpec((CHUNK // 2, n_left, 2, width, ff), lambda i: (i, which // n_left, 0, 0, 0))],
        out_specs=pl.BlockSpec((8, n_tok, width), lambda i: (0, 0, 0)),
        scratch_shapes=[pltpu.VMEM((CHUNK, rows, width), BF16)],
        compiler_params=local_params())(pos, *gate_parts, *lefts, weights)


def backward_kernel(pos, gate, dy_all, w_out, recv, pre_gate, pre_up, hidden, pack, d_gate, d_up, grad_in):
    for s in range(8):
        sel = one_hot(pos, s).astype(BF16)
        gate_slot = jnp.sum(one_hot(pos, s, gate), axis=1, keepdims=True)
        rows = (gate_slot * nn(sel, dy_all[s])).astype(BF16)
        for e in range(CHUNK):
            grad_in[e, s * SLOT:(s + 1) * SLOT, :] = rows[e * SLOT:(e + 1) * SLOT]
    for e in range(CHUNK):
        c = grad_in[e]
        d_hidden = nn(c, w_out[e // 2, 0, e % 2])
        act, slope = silu_parts(pre_gate[e])
        da = (d_hidden * pre_up[e] * slope).astype(BF16)
        db = (d_hidden * act).astype(BF16)
        d_gate[e] = da
        d_up[e] = db
        both = tn(recv[e], jnp.concatenate([da, db], axis=1)).astype(BF16)
        pack[e // 2, 0, e % 2] = both[:, :128]
        pack[e // 2, 1, e % 2] = both[:, 128:]
        pack[e // 2, 2, e % 2] = tn(c, hidden[e]).astype(BF16)


def expert_backward(pos, gate, dy_all, weights, recv, pre_gate, pre_up, hidden):
    _, n_mine, n_tok = pos.shape
    width, ff = weights.shape[3:]
    rows = 8 * SLOT
    per = lambda last: pl.BlockSpec((CHUNK, rows, last), lambda i: (i, 0, 0))
    return pl.pallas_call(
        backward_kernel, name='expert_backward', grid=(n_mine // CHUNK,),
        out_shape=[jax.ShapeDtypeStruct(weights.shape, BF16),
                   jax.ShapeDtypeStruct((n_mine, rows, ff), BF16),
                   jax.ShapeDtypeStruct((n_mine, rows, ff), BF16)],
        in_specs=[route_spec_of(n_tok)] * 2 + [pl.BlockSpec(dy_all.shape, lambda i: (0, 0, 0)),
                  pl.BlockSpec((CHUNK // 2, 1, 2, width, ff), lambda i: (i, 2, 0, 0, 0)),
                  per(width), per(ff), per(ff), per(ff)],
        out_specs=[pl.BlockSpec((CHUNK // 2, 3, 2, width, ff), lambda i: (i, 0, 0, 0, 0)), per(ff), per(ff)],
        scratch_shapes=[pltpu.VMEM((CHUNK, rows, width), BF16)],
        compiler_params=local_params())(pos, gate, dy_all, weights, recv, pre_gate, pre_up, hidden)


def routing(ids, gates, my_experts):
    hit = ids[:, None, :, :] == my_experts[None, :, None, None]
    used = jnp.any(hit, axis=3)
    gate_et = jnp.sum(jnp.where(hit, gates[:, None, :, :], 0.0), axis=3)
    n_tok = ids.shape[1]
    row = lax.broadcasted_iota(jnp.int32, (n_tok, n_tok), 0)
    col = lax.broadcasted_iota(jnp.int32, (n_tok, n_tok), 1)
    pos = dot('sit,tu->siu', used.astype(BF16), (row < col).astype(BF16))
    return jnp.where(used, pos, -1.0), gate_et


def solution(mesh):
    m4 = Mesh(mesh.devices.reshape(4, 4, 4, 2), ('z', 'y', 'x', 'dp'))
    ep = ('z', 'y', 'x')
    tok_spec = P(('dp',) + ep, None)
    route_spec = P(None, ('dp',) + ep, None)
    whole_spec = P(None, None, None)
    expert_spec = P(None, ep, None, None)

    def device_body(tokens, d_out, expert_ids, gate_vals, w_mix, w_gate, w_up, w_down):
        n_layers = w_mix.shape[0]
        n_chip = w_gate.shape[1]
        n_half = n_chip // 2
        tok_local, d_model = tokens.shape
        ff = w_gate.shape[3]
        top_k = expert_ids.shape[2]
        dp = lax.axis_index('dp')
        zi = lax.axis_index('z')
        n_mine = 16 * n_half
        loc = jnp.arange(n_mine, dtype=jnp.int32)
        my_experts = (zi * 16 + loc // n_half) * n_chip + dp * n_half + loc % n_half

        def gather_weights(layer):
            wg = lax.dynamic_slice_in_dim(w_gate[layer], dp * n_half, n_half, 0)
            wu = lax.dynamic_slice_in_dim(w_up[layer], dp * n_half, n_half, 0)
            wd = lax.dynamic_slice_in_dim(w_down[layer], dp * n_half, n_half, 0)
            pack = jnp.stack([wg, wu, jnp.swapaxes(wd, 1, 2)], axis=0)
            pack = pack.reshape(3 * n_half * d_model, ff)
            full = lax.all_gather(pack, ('y', 'x'), axis=0, tiled=False)
            return full.reshape(16, 3, n_half, d_model, ff)

        def scatter_grads(pack):
            part = lax.psum_scatter(pack.reshape(16 * 3 * n_half * d_model, ff), ('y', 'x'),
                                    scatter_dimension=0, tiled=True)
            return part

        def finish_grads(part):
            other = lax.ppermute(part, 'dp', [(0, 1), (1, 0)])
            lo = jnp.where(dp == 0, part, other).reshape(3, n_half, d_model, ff)
            hi = jnp.where(dp == 0, other, part).reshape(3, n_half, d_model, ff)
            both = jnp.concatenate([lo, hi], axis=1)
            return both[0], both[1], jnp.swapaxes(both[2], 1, 2)

        weights = [gather_weights(layer) for layer in range(n_layers)]

        route_pack = []
        for layer in range(n_layers):
            route_pack.append(expert_ids[layer].astype(BF16))
            route_pack.extend(part.astype(BF16) for part in split3(gate_vals[layer]))
        route_pack = jnp.concatenate(route_pack, axis=1)

        u_act = (tokens.astype(F32) + dot('td,de->te', tokens, w_mix[0])).astype(BF16)
        pad = route_pack.shape[1]
        first = jnp.concatenate([jnp.concatenate([u_act, route_pack], axis=1),
                                 jnp.pad(d_out, ((0, 0), (0, pad)))], axis=0)
        got = gather_line(first, 1)
        u_all = got[:, :tok_local, :d_model]
        dy_all = got[:, tok_local:, :d_model]
        r_all = got[:, :tok_local, d_model:]
        routes = []
        for layer in range(n_layers):
            seg = r_all[:, :, layer * 4 * top_k:(layer + 1) * 4 * top_k]
            ids = seg[:, :, :top_k].astype(jnp.int32)
            gates = (seg[:, :, top_k:2 * top_k].astype(F32) + seg[:, :, 2 * top_k:3 * top_k].astype(F32)
                     + seg[:, :, 3 * top_k:].astype(F32))
            pos, gate = routing(ids, gates, my_experts)
            routes.append((pos, gate, split3(gate)))

        layer_in = tokens
        saved = []
        for layer in range(n_layers):
            pos, gate, parts = routes[layer]
            if layer > 0:
                weights[layer], u_all = lax.optimization_barrier((weights[layer], u_all))
            state = expert_forward(pos, u_all, weights[layer])
            saved.append((layer_in, u_act, state))
            if layer < n_layers - 1:
                part = expert_combine(pos, parts, state[3:], weights[layer], 2)
                layer_in, u_act, u_all = pass_line(part, u_act, w_mix[layer + 1], False, True, 2 + layer)

        d_y = d_out
        mix_grads = []
        grads = []
        for layer in reversed(range(n_layers)):
            x_in, u_act, state = saved[layer]
            pos, gate, parts = routes[layer]
            pack, d_gate, d_up = expert_backward(pos, gate, dy_all, weights[layer], *state)
            grads.insert(0, scatter_grads(pack))
            part = expert_combine(pos, parts, (d_gate, d_up), weights[layer], 0)
            if layer > 0:
                d_u, d_y, dy_all = pass_line(part, d_y, w_mix[layer], True, True, 4 + layer)
            else:
                d_u, d_y = pass_line(part, d_y, w_mix[layer], True, False, 4)
            mix_grads.insert(0, dot('td,te->de', x_in, d_u).astype(BF16))
        x_in, u_act, state = saved[-1]
        pos, gate, parts = routes[-1]
        hidden, d_y = lax.optimization_barrier((state[3], d_y))
        layer_out = finish_line(expert_combine(pos, parts, (hidden,), weights[-1], 2), u_act, 6)
        mix_out = mix_sum(jnp.stack(mix_grads), 7)
        grads[1], layer_out = lax.optimization_barrier((grads[1], layer_out))
        grads = [finish_grads(part) for part in grads]
        return (layer_out, d_y, mix_out) + tuple(jnp.stack([g[k] for g in grads]) for k in range(3))

    return jax.shard_map(device_body, mesh=m4,
                         in_specs=(tok_spec, tok_spec, route_spec, route_spec, whole_spec,
                                   expert_spec, expert_spec, expert_spec),
                         out_specs=(tok_spec, tok_spec, whole_spec, expert_spec, expert_spec, expert_spec),
                         check_vma=False)
```

```python
import functools
import jax
import jax.numpy as jnp
from jax import lax
from jax.experimental import pallas as pl
from jax.experimental.pallas import tpu as pltpu
from jax.sharding import Mesh, PartitionSpec as P


F32 = jnp.float32
BF16 = jnp.bfloat16
MESH = pl.DeviceIdType.MESH
VMEM = pl.BlockSpec(memory_space=pltpu.VMEM)


def enter(peers):
    barrier = pltpu.get_barrier_semaphore()
    for peer in peers:
        pl.semaphore_signal(barrier, inc=1, device_id=peer, device_id_type=MESH)
    pl.semaphore_wait(barrier, len(peers))


def send(src, dst, send_sems, recv_sems, index, peer):
    copy = pltpu.make_async_remote_copy(src_ref=src, dst_ref=dst, send_sem=send_sems.at[index],
                                        recv_sem=recv_sems.at[index], device_id=peer, device_id_type=MESH)
    copy.start()
    return copy


def line_peers():
    z, dp = lax.axis_index('z'), lax.axis_index('dp')
    up, down = {'z': lax.rem(z + 1, 4)}, {'z': lax.rem(z + 3, 4)}
    return z, dp, up, down, {'dp': 1 - dp}


N_AG = 9


def line_gather(src, dst, send_sems, recv_sems, base):
    for _ in line_gather_steps(src, dst, send_sems, recv_sems, base):
        pass


def line_gather_steps(src, dst, send_sems, recv_sems, base):
    z, dp, up, down, mate = line_peers()
    rows = src.shape[0]
    half = rows // 2
    me = z * 2 + dp
    below, above = lax.rem(z + 3, 4) * 2 + dp, lax.rem(z + 1, 4) * 2 + dp
    far = lax.rem(z + 2, 4) * 2 + dp
    lo, hi = pl.ds(0, half), pl.ds(half, half)
    go = functools.partial(send, send_sems=send_sems, recv_sems=recv_sems)
    to_up = go(src, dst.at[me], index=base, peer=up)
    to_down = go(src, dst.at[me], index=base + 1, peer=down)
    to_mate = go(src, dst.at[me], index=base + 2, peer=mate)
    dst[me] = src[...]
    yield
    to_up.wait_recv()
    relay_up = go(dst.at[below, lo], dst.at[below, lo], index=base + 3, peer=up)
    mate_below = go(dst.at[below], dst.at[below], index=base + 5, peer=mate)
    to_down.wait_recv()
    relay_down = go(dst.at[above, hi], dst.at[above, hi], index=base + 4, peer=down)
    mate_above = go(dst.at[above], dst.at[above], index=base + 6, peer=mate)
    yield
    relay_up.wait_recv()
    mate_lo = go(dst.at[far, lo], dst.at[far, lo], index=base + 7, peer=mate)
    relay_down.wait_recv()
    mate_hi = go(dst.at[far, hi], dst.at[far, hi], index=base + 8, peer=mate)
    for copy in (to_mate, mate_below, mate_above, mate_lo, mate_hi):
        copy.wait_recv()
    for copy in (to_up, to_down, to_mate, relay_up, relay_down, mate_below, mate_above, mate_lo, mate_hi):
        copy.wait_send()


N_RS = 10


def line_reduce_steps(part, bufs, send_sems, recv_sems, base):
    d_part, sums, relay_lo, relay_hi, in_lo, in_hi = bufs
    z, dp, up, down, mate = line_peers()
    half = part.shape[1] // 2
    lo, hi = pl.ds(0, half), pl.ds(half, half)
    order = [lax.rem(z + 2, 4), lax.rem(z + 1, 4), lax.rem(z + 3, 4), z]
    go = functools.partial(send, send_sems=send_sems, recv_sems=recv_sems)
    swaps = [go(part.at[zk * 2 + 1 - dp], d_part.at[k], index=base + k, peer=mate) for k, zk in enumerate(order)]
    yield
    swaps[0].wait_recv()
    sums[0] = part[order[0] * 2 + dp] + d_part[0]
    far_up = go(sums.at[0, lo], relay_lo, index=base + 4, peer=up)
    far_down = go(sums.at[0, hi], relay_hi, index=base + 5, peer=down)
    swaps[1].wait_recv()
    sums[1] = part[order[1] * 2 + dp] + d_part[1]
    up_hi = go(sums.at[1, hi], in_lo.at[hi], index=base + 6, peer=up)
    swaps[2].wait_recv()
    sums[2] = part[order[2] * 2 + dp] + d_part[2]
    down_lo = go(sums.at[2, lo], in_hi.at[lo], index=base + 7, peer=down)
    swaps[3].wait_recv()
    sums[3] = part[order[3] * 2 + dp] + d_part[3]
    far_up.wait_recv()
    sums[1, lo] = sums[1, lo] + relay_lo[...]
    up_lo = go(sums.at[1, lo], in_lo.at[lo], index=base + 8, peer=up)
    far_down.wait_recv()
    sums[2, hi] = sums[2, hi] + relay_hi[...]
    down_hi = go(sums.at[2, hi], in_hi.at[hi], index=base + 9, peer=down)
    yield
    for copy in (up_hi, down_lo, up_lo, down_hi):
        copy.wait_recv()
    for copy in swaps + [far_up, far_down, up_hi, down_lo, up_lo, down_hi]:
        copy.wait_send()
    yield sums[3] + in_lo[...] + in_hi[...]


def line_reduce(part, bufs, send_sems, recv_sems, base):
    for total in line_reduce_steps(part, bufs, send_sems, recv_sems, base):
        pass
    return total


def reduce_scratch(tok, width):
    return [pltpu.VMEM((4, tok, width), F32), pltpu.VMEM((4, tok, width), F32),
            pltpu.VMEM((tok // 2, width), F32), pltpu.VMEM((tok // 2, width), F32),
            pltpu.VMEM((tok, width), F32), pltpu.VMEM((tok, width), F32)]


def params(collective_id):
    return pltpu.CompilerParams(collective_id=collective_id, has_side_effects=True,
                                vmem_limit_bytes=60 * 1024 * 1024)


def pass_kernel(transpose, want_all, part, base, w_mix, y_ref, next_ref, *rest):
    if want_all:
        all_ref, rest = rest[0], rest[1:]
    bufs, (send_sems, recv_sems) = rest[:-2], rest[-2:]
    _, _, up, down, mate = line_peers()
    enter((up, down, mate))
    total = line_reduce(part, bufs, send_sems, recv_sems, 0)
    y_val = (base[...].astype(F32) + total).astype(BF16)
    y_ref[...] = y_val
    contract = (((1,), (1 if transpose else 0,)), ((), ()))
    mixed = lax.dot_general(y_val, w_mix[...], contract, preferred_element_type=F32)
    next_ref[...] = (y_val.astype(F32) + mixed).astype(BF16)
    if want_all:
        line_gather(next_ref, all_ref, send_sems, recv_sems, N_RS)


def pass_line(part, base, w_mix, transpose, want_all, collective_id):
    _, tok, width = part.shape
    block = jax.ShapeDtypeStruct((tok, width), BF16)
    outs = [block, block] + ([jax.ShapeDtypeStruct((8, tok, width), BF16)] if want_all else [])
    n_sem = N_RS + (N_AG if want_all else 0)
    return pl.pallas_call(
        functools.partial(pass_kernel, transpose, want_all), name='pass_line',
        out_shape=outs, in_specs=[VMEM] * 3, out_specs=[VMEM] * len(outs),
        scratch_shapes=reduce_scratch(tok, width) + [pltpu.SemaphoreType.DMA((n_sem,)),
                                                     pltpu.SemaphoreType.DMA((n_sem,))],
        compiler_params=params(collective_id))(part, base, w_mix)


def mix_peers():
    at = {axis: lax.axis_index(axis) for axis in 'xyz'}
    return at, {axis: [{axis: lax.rem(at[axis] + k, 4)} for k in (1, 2, 3)] for axis in 'xyz'}


def mix_steps(grad, out, bufs, send_sems, recv_sems, base):
    dp = lax.axis_index('dp')
    mate = {'dp': 1 - dp}
    at, peers = mix_peers()
    mate_in, quarter_in, block, y_in, y_out, z_in, z_out = bufs
    quarter = grad.shape[1] // 4
    go = functools.partial(send, send_sems=send_sems, recv_sems=recv_sems)
    copies = []
    swap = go(grad.at[1 - dp], mate_in, index=base, peer=mate)
    yield
    swap.wait_recv()
    block[...] = (grad[dp].astype(F32) + mate_in[...].astype(F32)).astype(BF16)
    mine = pl.ds(pl.multiple_of(at['x'] * quarter, quarter), quarter)
    stage = []
    for k in range(3):
        rows = pl.ds(pl.multiple_of(lax.rem(at['x'] + k + 1, 4) * quarter, quarter), quarter)
        stage.append(go(block.at[rows], quarter_in.at[k], index=base + 1 + k, peer=peers['x'][k]))
    copies += [swap] + stage
    yield
    total = block[mine].astype(F32)
    for k in range(3):
        stage[k].wait_recv()
        total = total + quarter_in[k].astype(F32)
    for axis, buf_in, buf_out, first in (('y', y_in, y_out, base + 4), ('z', z_in, z_out, base + 7)):
        buf_out[...] = total.astype(BF16)
        stage = [go(buf_out, buf_in.at[k], index=first + k, peer=peers[axis][k]) for k in range(3)]
        copies += stage
        terms = [buf_out[...].astype(F32)]
        for k in range(3):
            stage[k].wait_recv()
            terms.append(buf_in[k].astype(F32))
        here = at[axis]
        total = None
        for coord in range(4):
            term = jnp.zeros_like(terms[0])
            for k in range(4):
                source = lax.rem(here + 4 - k, 4)
                term = jnp.where(source == coord, terms[k], term)
            total = term if total is None else total + term
    final = total.astype(BF16)
    out[dp, mine] = final
    stage = [go(out.at[dp, mine], out.at[dp, mine], index=base + 10 + k, peer=peers['x'][k]) for k in range(3)]
    copies += stage
    for k in range(3):
        stage[k].wait_recv()
    swap = go(out.at[dp], out.at[dp], index=base + 13, peer=mate)
    swap.wait_recv()
    copies.append(swap)
    for copy in copies:
        copy.wait_send()
    yield


N_MIX = 14


def close_kernel(part_v, base_v, w_mix, x_in, mix_top, part_y, base_y, dx_ref, y_ref, mix_ref, *scratch):
    bufs_v, bufs_y, bufs_m = scratch[:6], scratch[6:12], scratch[12:19]
    grad, send_sems, recv_sems = scratch[19:]
    _, _, _, _, mate = line_peers()
    _, peers = mix_peers()
    enter(peers['x'] + peers['y'] + peers['z'] + [mate])
    steps_v = line_reduce_steps(part_v, bufs_v, send_sems, recv_sems, 0)
    steps_y = line_reduce_steps(part_y, bufs_y, send_sems, recv_sems, N_RS)
    steps_m = mix_steps(grad, mix_ref, bufs_m, send_sems, recv_sems, 2 * N_RS)
    next(steps_v)
    next(steps_y)
    grad[1] = mix_top[...]
    next(steps_v)
    d_u = (base_v[...].astype(F32) + next(steps_v)).astype(BF16)
    grad[0] = tn(x_in[...], d_u).astype(BF16)
    next(steps_m)
    dx_ref[...] = (d_u.astype(F32) + nt(d_u, w_mix[...])).astype(BF16)
    next(steps_m)
    next(steps_y)
    next(steps_m)
    y_ref[...] = (base_y[...].astype(F32) + next(steps_y)).astype(BF16)


def close_line(part_v, base_v, w_mix, x_in, mix_top, part_y, base_y, collective_id):
    _, tok, width = part_v.shape
    quarter = width // 4
    n_sem = 2 * N_RS + N_MIX
    block = jax.ShapeDtypeStruct((tok, width), BF16)
    return pl.pallas_call(
        close_kernel, name='close_line',
        out_shape=[block, block, jax.ShapeDtypeStruct((2, width, width), BF16)],
        in_specs=[VMEM] * 7, out_specs=[VMEM] * 3,
        scratch_shapes=reduce_scratch(tok, width) * 2
        + [pltpu.VMEM((width, width), BF16), pltpu.VMEM((3, quarter, width), BF16), pltpu.VMEM((width, width), BF16)]
        + [pltpu.VMEM((3, quarter, width), BF16), pltpu.VMEM((quarter, width), BF16)] * 2
        + [pltpu.VMEM((2, width, width), BF16), pltpu.SemaphoreType.DMA((n_sem,)), pltpu.SemaphoreType.DMA((n_sem,))],
        compiler_params=params(collective_id))(part_v, base_v, w_mix, x_in, mix_top, part_y, base_y)


N_PLANE = 40


def plane_gather_steps(src, dst, send_sems, recv_sems, base):
    at = {axis: lax.axis_index(axis) for axis in 'xy'}
    rows = src.shape[2] // 2
    part = (pl.ds(0, rows), pl.ds(rows, rows))
    go = functools.partial(send, send_sems=send_sems, recv_sems=recv_sems)
    copies = []

    def block(half, i, j):
        dx, dy = (i, j) if half == 0 else (j, i)
        return lax.rem(at['y'] + dy + 4, 4) * 4 + lax.rem(at['x'] + dx + 4, 4)

    def peer(half, stage, step):
        axis = 'xy'[stage] if half == 0 else 'yx'[stage]
        return {axis: lax.rem(at[axis] + step + 4, 4)}

    counter = [base]

    def launch(half, stage, step, i, j, rows_of=None, own=False):
        b = block(half, i, j)
        to = dst.at[b, :, half] if rows_of is None else dst.at[b, :, half, part[rows_of]]
        copy = go(src.at[:, half] if own else to, to, index=counter[0], peer=peer(half, stage, step))
        counter[0] += 1
        copies.append(copy)
        return copy

    first, second, relay1, relay2 = {}, {}, {}, {}
    for half in (0, 1):
        for step in (1, -1):
            first[half, step] = launch(half, 0, step, 0, 0, own=True)
    for half in (0, 1):
        for step in (1, -1):
            second[half, 0, step] = launch(half, 1, step, 0, 0, own=True)
    dst[at['y'] * 4 + at['x']] = src[...]
    yield
    for step in (1, -1):
        for half in (0, 1):
            first[half, step].wait_recv()
            relay1[half, step] = launch(half, 0, step, -step, 0, rows_of=0 if step == 1 else 1)
            for out in (1, -1):
                second[half, -step, out] = launch(half, 1, out, -step, 0)
    yield

    def forward(i):
        for step in (1, -1):
            for half in (0, 1):
                second[half, i, step].wait_recv()
                relay2[half, i, step] = launch(half, 1, step, i, -step, rows_of=0 if step == 1 else 1)

    forward(0)
    for half in (0, 1):
        for step in (1, -1):
            relay1[half, step].wait_recv()
        for out in (1, -1):
            second[half, 2, out] = launch(half, 1, out, 2, 0)
    yield
    forward(-1)
    forward(1)
    forward(2)
    for copy in relay2.values():
        copy.wait_recv()
    for copy in copies:
        copy.wait_send()
    yield


def open_kernel(n_chip, tok_src, route_src, w_src, tok_all, route, w_all, route_all, send_sems, recv_sems):
    z, dp, up, down, mate = line_peers()
    at = {axis: lax.axis_index(axis) for axis in 'xy'}
    enter([up, down, mate] + [{axis: lax.rem(at[axis] + k, 4)} for axis in 'xy' for k in (1, 3)])
    steps_w = plane_gather_steps(w_src, w_all, send_sems, recv_sems, 0)
    steps_r = line_gather_steps(route_src, route_all, send_sems, recv_sems, N_PLANE)
    steps_t = line_gather_steps(tok_src, tok_all, send_sems, recv_sems, N_PLANE + N_AG)
    next(steps_w)
    next(steps_r)
    next(steps_t)
    for steps in (steps_r, steps_w, steps_t):
        next(steps)
    next(steps_w)
    for steps in (steps_r, steps_t):
        for _ in steps:
            pass
    n_layers, _, _, n_mine, n_tok = route.shape
    n_half = n_chip // 2
    loc = lax.broadcasted_iota(jnp.int32, (n_mine, n_tok), 0)
    mine = ((z * 16 + loc // n_half) * n_chip + dp * n_half + lax.rem(loc, n_half)).astype(F32)
    row = lax.broadcasted_iota(jnp.int32, (n_tok, n_tok), 0)
    col = lax.broadcasted_iota(jnp.int32, (n_tok, n_tok), 1)
    before = jnp.where(row < col, 1.0, 0.0).astype(BF16)
    top_k = route_src.shape[0] // (4 * n_layers)
    for layer in range(n_layers):
        for s in range(8):
            rows = route_all[s, layer * 4 * top_k:(layer + 1) * 4 * top_k, :].astype(F32)
            used = jnp.zeros((n_mine, n_tok), F32)
            gates = [jnp.zeros((n_mine, n_tok), F32) for _ in range(3)]
            for j in range(top_k):
                hit = jnp.broadcast_to(rows[j:j + 1], mine.shape) == mine
                used = jnp.where(hit, 1.0, used)
                for k in range(3):
                    val = rows[(k + 1) * top_k + j:(k + 1) * top_k + j + 1]
                    gates[k] = jnp.where(hit, jnp.broadcast_to(val, mine.shape), gates[k])
            pos = nn(used.astype(BF16), before)
            route[layer, 0, s] = jnp.where(used > 0.5, pos, -1.0)
            for k in range(3):
                route[layer, 1 + k, s] = gates[k]
    for _ in steps_w:
        pass


def open_line(tok_src, route_src, w_src, n_layers, n_chip, collective_id):
    n_tok = route_src.shape[1]
    n_mine = 16 * n_chip // 2
    n_sem = N_PLANE + 2 * N_AG
    return pl.pallas_call(
        functools.partial(open_kernel, n_chip), name='open_line',
        out_shape=[jax.ShapeDtypeStruct((8,) + tok_src.shape, BF16),
                   jax.ShapeDtypeStruct((n_layers, 4, 8, n_mine, n_tok), F32),
                   jax.ShapeDtypeStruct((16,) + w_src.shape, BF16)],
        in_specs=[VMEM] * 3, out_specs=[VMEM] * 3,
        scratch_shapes=[pltpu.VMEM((8,) + route_src.shape, BF16),
                        pltpu.SemaphoreType.DMA((n_sem,)), pltpu.SemaphoreType.DMA((n_sem,))],
        compiler_params=params(collective_id))(tok_src, route_src, w_src)


def silu_parts(pre_gate):
    sig_val = jax.nn.sigmoid(pre_gate)
    return pre_gate * sig_val, sig_val * (1.0 + pre_gate * (1.0 - sig_val))


def split3(val):
    hi = lax.reduce_precision(val, 8, 7)
    rest = val - hi
    mid = lax.reduce_precision(rest, 8, 7)
    return hi, mid, rest - mid


def dot(spec, a, b):
    return jnp.einsum(spec, a, b, preferred_element_type=F32)


CHUNK = 8
SLOT = 32


def pick(pos_row, slots):
    return jnp.broadcast_to(pos_row, slots.shape) == slots


def one_hot(pos, source, values=None):
    n_tok = pos.shape[2]
    slots = lax.broadcasted_iota(jnp.int32, (SLOT, n_tok), 0).astype(F32)
    blocks = []
    for e in range(CHUNK):
        mask = pick(pos[source, e:e + 1, :], slots)
        val = 1.0 if values is None else jnp.broadcast_to(values[e:e + 1], mask.shape)
        blocks.append(jnp.where(mask, val, 0.0))
    return jnp.concatenate(blocks, axis=0)


def nn(a, b):
    return lax.dot_general(a, b, (((1,), (0,)), ((), ())), preferred_element_type=F32)


def nt(a, b):
    return lax.dot_general(a, b, (((1,), (1,)), ((), ())), preferred_element_type=F32)


def tn(a, b):
    return lax.dot_general(a, b, (((0,), (0,)), ((), ())), preferred_element_type=F32)


def forward_kernel(pos, u_all, w_in, recv, pre_gate, pre_up, hidden):
    for s in range(8):
        rows = nn(one_hot(pos, s).astype(BF16), u_all[s]).astype(BF16)
        for e in range(CHUNK):
            recv[e, s * SLOT:(s + 1) * SLOT, :] = rows[e * SLOT:(e + 1) * SLOT]
    for e in range(CHUNK):
        w_both = jnp.concatenate([w_in[e // 2, 0, e % 2], w_in[e // 2, 1, e % 2]], axis=1)
        both = nn(recv[e], w_both)
        a, b = both[:, :128], both[:, 128:]
        act, _ = silu_parts(a)
        pre_gate[e] = a
        pre_up[e] = b
        hidden[e] = (act * b).astype(BF16)


def route_specs(route, layer, kinds):
    return [pl.BlockSpec((None, None, 8, CHUNK, route.shape[4]), lambda i, k=k: (layer, k, 0, i, 0)) for k in kinds]


def token_spec(tok_all, n_tok, part):
    return pl.BlockSpec((8, n_tok, tok_all.shape[2]), lambda i: (0, part, 0))


def local_params():
    return pltpu.CompilerParams(vmem_limit_bytes=60 * 1024 * 1024)


def expert_forward(route, layer, u_all, weights):
    n_mine, n_tok = route.shape[3:]
    width = u_all.shape[2]
    ff = weights.shape[4]
    rows = 8 * SLOT
    per = lambda last: pl.BlockSpec((CHUNK, rows, last), lambda i: (i, 0, 0))
    return pl.pallas_call(
        forward_kernel, name='expert_forward', grid=(n_mine // CHUNK,),
        out_shape=[jax.ShapeDtypeStruct((n_mine, rows, width), BF16),
                   jax.ShapeDtypeStruct((n_mine, rows, ff), F32),
                   jax.ShapeDtypeStruct((n_mine, rows, ff), F32),
                   jax.ShapeDtypeStruct((n_mine, rows, ff), BF16)],
        in_specs=route_specs(route, layer, (0,)) + [
                  token_spec(u_all, n_tok, 0),
                  pl.BlockSpec((CHUNK // 2, 2, 2, width, ff), lambda i: (i, 0, 0, 0, 0))],
        out_specs=[per(width), per(ff), per(ff), per(ff)],
        compiler_params=local_params())(route, u_all, weights)


def combine_kernel(n_left, pos, hi, mid, lo, *refs):
    lefts, w_out, part, rows = refs[:n_left], refs[n_left], refs[n_left + 1], refs[n_left + 2]
    for e in range(CHUNK):
        left = jnp.concatenate([ref[e] for ref in lefts], axis=1)
        right = jnp.concatenate([w_out[e // 2, k, e % 2] for k in range(n_left)], axis=1)
        rows[e] = nt(left, right).astype(BF16)
    for s in range(8):
        mine = jnp.concatenate([rows[e, s * SLOT:(s + 1) * SLOT, :] for e in range(CHUNK)], axis=0)
        val = tn(one_hot(pos, s, lo[s]).astype(BF16), mine)
        val = val + tn(one_hot(pos, s, mid[s]).astype(BF16), mine)
        val = val + tn(one_hot(pos, s, hi[s]).astype(BF16), mine)

        @pl.when(pl.program_id(0) == 0)
        def _(val=val, s=s):
            part[s] = val

        @pl.when(pl.program_id(0) > 0)
        def _(val=val, s=s):
            part[s] = part[s] + val


def expert_combine(route, layer, lefts, weights, which):
    n_mine, n_tok = route.shape[3:]
    width, ff = weights.shape[3:]
    rows = 8 * SLOT
    n_left = len(lefts)
    per = pl.BlockSpec((CHUNK, rows, ff), lambda i: (i, 0, 0))
    return pl.pallas_call(
        functools.partial(combine_kernel, n_left), name='expert_combine', grid=(n_mine // CHUNK,),
        out_shape=jax.ShapeDtypeStruct((8, n_tok, width), F32),
        in_specs=route_specs(route, layer, (0, 1, 2, 3)) + [per] * n_left
        + [pl.BlockSpec((CHUNK // 2, n_left, 2, width, ff), lambda i: (i, which // n_left, 0, 0, 0))],
        out_specs=pl.BlockSpec((8, n_tok, width), lambda i: (0, 0, 0)),
        scratch_shapes=[pltpu.VMEM((CHUNK, rows, width), BF16)],
        compiler_params=local_params())(*[route] * 4, *lefts, weights)


def backward_kernel(pos, hi, mid, lo, dy_all, w_out, recv, pre_gate, pre_up, hidden, pack, d_gate, d_up, grad_in):
    for s in range(8):
        sel = one_hot(pos, s).astype(BF16)
        gate_slot = jnp.sum(one_hot(pos, s, (hi[s] + mid[s]) + lo[s]), axis=1, keepdims=True)
        rows = (gate_slot * nn(sel, dy_all[s])).astype(BF16)
        for e in range(CHUNK):
            grad_in[e, s * SLOT:(s + 1) * SLOT, :] = rows[e * SLOT:(e + 1) * SLOT]
    for e in range(CHUNK):
        c = grad_in[e]
        d_hidden = nn(c, w_out[e // 2, 0, e % 2])
        act, slope = silu_parts(pre_gate[e])
        da = (d_hidden * pre_up[e] * slope).astype(BF16)
        db = (d_hidden * act).astype(BF16)
        d_gate[e] = da
        d_up[e] = db
        both = tn(recv[e], jnp.concatenate([da, db], axis=1)).astype(BF16)
        pack[e // 2, 0, e % 2] = both[:, :128]
        pack[e // 2, 1, e % 2] = both[:, 128:]
        pack[e // 2, 2, e % 2] = tn(c, hidden[e]).astype(BF16)


def expert_backward(route, layer, dy_all, part, weights, recv, pre_gate, pre_up, hidden):
    n_mine, n_tok = route.shape[3:]
    width, ff = weights.shape[3:]
    rows = 8 * SLOT
    per = lambda last: pl.BlockSpec((CHUNK, rows, last), lambda i: (i, 0, 0))
    return pl.pallas_call(
        backward_kernel, name='expert_backward', grid=(n_mine // CHUNK,),
        out_shape=[jax.ShapeDtypeStruct(weights.shape, BF16),
                   jax.ShapeDtypeStruct((n_mine, rows, ff), BF16),
                   jax.ShapeDtypeStruct((n_mine, rows, ff), BF16)],
        in_specs=route_specs(route, layer, (0, 1, 2, 3)) + [
                  token_spec(dy_all, n_tok, part),
                  pl.BlockSpec((CHUNK // 2, 1, 2, width, ff), lambda i: (i, 2, 0, 0, 0)),
                  per(width), per(ff), per(ff), per(ff)],
        out_specs=[pl.BlockSpec((CHUNK // 2, 3, 2, width, ff), lambda i: (i, 0, 0, 0, 0)), per(ff), per(ff)],
        scratch_shapes=[pltpu.VMEM((CHUNK, rows, width), BF16)],
        compiler_params=local_params())(*[route] * 4, dy_all, weights, recv, pre_gate, pre_up, hidden)


def solution(mesh):
    m4 = Mesh(mesh.devices.reshape(4, 4, 4, 2), ('z', 'y', 'x', 'dp'))
    ep = ('z', 'y', 'x')
    tok_spec = P(('dp',) + ep, None)
    route_spec = P(None, ('dp',) + ep, None)
    whole_spec = P(None, None, None)
    expert_spec = P(None, ep, None, None)

    def device_body(tokens, d_out, expert_ids, gate_vals, w_mix, w_gate, w_up, w_down):
        n_layers = w_mix.shape[0]
        n_chip = w_gate.shape[1]
        n_half = n_chip // 2
        _, d_model = tokens.shape
        ff = w_gate.shape[3]
        dp = lax.axis_index('dp')

        def own_weights(layer):
            wg = lax.dynamic_slice_in_dim(w_gate[layer], dp * n_half, n_half, 0)
            wu = lax.dynamic_slice_in_dim(w_up[layer], dp * n_half, n_half, 0)
            wd = lax.dynamic_slice_in_dim(w_down[layer], dp * n_half, n_half, 0)
            return jnp.stack([wg, wu, jnp.swapaxes(wd, 1, 2)], axis=0)

        def scatter_grads(pack):
            part = lax.psum_scatter(pack.reshape(16 * 3 * n_half * d_model, ff), ('y', 'x'),
                                    scatter_dimension=0, tiled=True)
            return part

        def finish_grads(part):
            other = lax.ppermute(part, 'dp', [(0, 1), (1, 0)])
            lo = jnp.where(dp == 0, part, other).reshape(3, n_half, d_model, ff)
            hi = jnp.where(dp == 0, other, part).reshape(3, n_half, d_model, ff)
            both = jnp.concatenate([lo, hi], axis=1)
            return both[0], both[1], jnp.swapaxes(both[2], 1, 2)

        route_src = []
        for layer in range(n_layers):
            route_src.append(expert_ids[layer].astype(BF16))
            route_src.extend(part.astype(BF16) for part in split3(gate_vals[layer]))
        route_src = jnp.concatenate(route_src, axis=1).T

        u_act = (tokens.astype(F32) + dot('td,de->te', tokens, w_mix[0])).astype(BF16)
        first = jnp.concatenate([u_act, d_out], axis=0)
        tok_all, route, w_first = open_line(first, route_src, own_weights(0), n_layers, n_chip, 1)
        own_top, w_first = lax.optimization_barrier((own_weights(1), w_first))
        w_top = lax.all_gather(own_top.reshape(3 * n_half * d_model, ff), ('y', 'x'), axis=0, tiled=False)
        w_top = w_top.reshape(16, 3, n_half, d_model, ff)

        low = expert_forward(route, 0, tok_all, w_first)
        part = expert_combine(route, 0, low[3:], w_first, 2)
        y_low, u_top, u_all = pass_line(part, u_act, w_mix[1], False, True, 2)

        w_top, u_all = lax.optimization_barrier((w_top, u_all))
        top = expert_forward(route, 1, u_all, w_top)
        pack, d_gate, d_up = expert_backward(route, 1, tok_all, 1, w_top, *top)
        grad_top = scatter_grads(pack)
        part = expert_combine(route, 1, (d_gate, d_up), w_top, 0)
        d_u, d_y, dy_all = pass_line(part, d_out, w_mix[1], True, True, 3)
        mix_top = dot('td,te->de', y_low, d_u).astype(BF16)

        pack, d_gate, d_up = expert_backward(route, 0, dy_all, 0, w_first, *low)
        grad_low = scatter_grads(pack)
        part_v = expert_combine(route, 0, (d_gate, d_up), w_first, 0)
        hidden, part_v = lax.optimization_barrier((top[3], part_v))
        part_y = expert_combine(route, 1, (hidden,), w_top, 2)
        d_tokens, layer_out, mix_out = close_line(part_v, d_y, w_mix[0], tokens, mix_top, part_y, u_top, 4)
        grad_top, d_tokens = lax.optimization_barrier((grad_top, d_tokens))
        grads = [finish_grads(grad_low), finish_grads(grad_top)]
        return (layer_out, d_tokens, mix_out) + tuple(jnp.stack([g[k] for g in grads]) for k in range(3))

    return jax.shard_map(device_body, mesh=m4,
                         in_specs=(tok_spec, tok_spec, route_spec, route_spec, whole_spec,
                                   expert_spec, expert_spec, expert_spec),
                         out_specs=(tok_spec, tok_spec, whole_spec, expert_spec, expert_spec, expert_spec),
                         check_vma=False)
```

```python
import functools
import jax
import jax.numpy as jnp
from jax import lax
from jax.experimental import pallas as pl
from jax.experimental.pallas import tpu as pltpu
from jax.sharding import Mesh, PartitionSpec as P


F32 = jnp.float32
BF16 = jnp.bfloat16
MESH = pl.DeviceIdType.MESH
VMEM = pl.BlockSpec(memory_space=pltpu.VMEM)


def enter(peers):
    barrier = pltpu.get_barrier_semaphore()
    for peer in peers:
        pl.semaphore_signal(barrier, inc=1, device_id=peer, device_id_type=MESH)
    pl.semaphore_wait(barrier, len(peers))


def send(src, dst, send_sems, recv_sems, index, peer):
    copy = pltpu.make_async_remote_copy(src_ref=src, dst_ref=dst, send_sem=send_sems.at[index],
                                        recv_sem=recv_sems.at[index], device_id=peer, device_id_type=MESH)
    copy.start()
    return copy


def line_peers():
    z, dp = lax.axis_index('z'), lax.axis_index('dp')
    up, down = {'z': lax.rem(z + 1, 4)}, {'z': lax.rem(z + 3, 4)}
    return z, dp, up, down, {'dp': 1 - dp}


N_AG = 9


def line_gather(src, dst, send_sems, recv_sems, base):
    for _ in line_gather_steps(src, dst, send_sems, recv_sems, base):
        pass


def line_gather_steps(src, dst, send_sems, recv_sems, base):
    z, dp, up, down, mate = line_peers()
    rows = src.shape[0]
    half = rows // 2
    me = z * 2 + dp
    below, above = lax.rem(z + 3, 4) * 2 + dp, lax.rem(z + 1, 4) * 2 + dp
    far = lax.rem(z + 2, 4) * 2 + dp
    lo, hi = pl.ds(0, half), pl.ds(half, half)
    go = functools.partial(send, send_sems=send_sems, recv_sems=recv_sems)
    to_up = go(src, dst.at[me], index=base, peer=up)
    to_down = go(src, dst.at[me], index=base + 1, peer=down)
    to_mate = go(src, dst.at[me], index=base + 2, peer=mate)
    dst[me] = src[...]
    yield
    to_up.wait_recv()
    relay_up = go(dst.at[below, lo], dst.at[below, lo], index=base + 3, peer=up)
    mate_below = go(dst.at[below], dst.at[below], index=base + 5, peer=mate)
    to_down.wait_recv()
    relay_down = go(dst.at[above, hi], dst.at[above, hi], index=base + 4, peer=down)
    mate_above = go(dst.at[above], dst.at[above], index=base + 6, peer=mate)
    yield
    relay_up.wait_recv()
    mate_lo = go(dst.at[far, lo], dst.at[far, lo], index=base + 7, peer=mate)
    relay_down.wait_recv()
    mate_hi = go(dst.at[far, hi], dst.at[far, hi], index=base + 8, peer=mate)
    for copy in (to_mate, mate_below, mate_above, mate_lo, mate_hi):
        copy.wait_recv()
    for copy in (to_up, to_down, to_mate, relay_up, relay_down, mate_below, mate_above, mate_lo, mate_hi):
        copy.wait_send()


N_RS = 10


def line_reduce_steps(part, bufs, send_sems, recv_sems, base):
    d_part, sums, relay_lo, relay_hi, in_lo, in_hi = bufs
    z, dp, up, down, mate = line_peers()
    half = part.shape[1] // 2
    lo, hi = pl.ds(0, half), pl.ds(half, half)
    order = [lax.rem(z + 2, 4), lax.rem(z + 1, 4), lax.rem(z + 3, 4), z]
    go = functools.partial(send, send_sems=send_sems, recv_sems=recv_sems)
    swaps = [go(part.at[zk * 2 + 1 - dp], d_part.at[k], index=base + k, peer=mate) for k, zk in enumerate(order)]
    yield
    swaps[0].wait_recv()
    sums[0] = part[order[0] * 2 + dp] + d_part[0]
    far_up = go(sums.at[0, lo], relay_lo, index=base + 4, peer=up)
    far_down = go(sums.at[0, hi], relay_hi, index=base + 5, peer=down)
    swaps[1].wait_recv()
    sums[1] = part[order[1] * 2 + dp] + d_part[1]
    up_hi = go(sums.at[1, hi], in_lo.at[hi], index=base + 6, peer=up)
    swaps[2].wait_recv()
    sums[2] = part[order[2] * 2 + dp] + d_part[2]
    down_lo = go(sums.at[2, lo], in_hi.at[lo], index=base + 7, peer=down)
    swaps[3].wait_recv()
    sums[3] = part[order[3] * 2 + dp] + d_part[3]
    far_up.wait_recv()
    sums[1, lo] = sums[1, lo] + relay_lo[...]
    up_lo = go(sums.at[1, lo], in_lo.at[lo], index=base + 8, peer=up)
    far_down.wait_recv()
    sums[2, hi] = sums[2, hi] + relay_hi[...]
    down_hi = go(sums.at[2, hi], in_hi.at[hi], index=base + 9, peer=down)
    yield
    for copy in (up_hi, down_lo, up_lo, down_hi):
        copy.wait_recv()
    for copy in swaps + [far_up, far_down, up_hi, down_lo, up_lo, down_hi]:
        copy.wait_send()
    yield sums[3] + in_lo[...] + in_hi[...]


def line_reduce(part, bufs, send_sems, recv_sems, base):
    for total in line_reduce_steps(part, bufs, send_sems, recv_sems, base):
        pass
    return total


def reduce_scratch(tok, width):
    return [pltpu.VMEM((4, tok, width), F32), pltpu.VMEM((4, tok, width), F32),
            pltpu.VMEM((tok // 2, width), F32), pltpu.VMEM((tok // 2, width), F32),
            pltpu.VMEM((tok, width), F32), pltpu.VMEM((tok, width), F32)]


def params(collective_id):
    return pltpu.CompilerParams(collective_id=collective_id, has_side_effects=True,
                                vmem_limit_bytes=60 * 1024 * 1024)


def pass_kernel(transpose, want_all, part, base, w_mix, y_ref, next_ref, *rest):
    if want_all:
        all_ref, rest = rest[0], rest[1:]
    bufs, (send_sems, recv_sems) = rest[:-2], rest[-2:]
    _, _, up, down, mate = line_peers()
    enter((up, down, mate))
    total = line_reduce(part, bufs, send_sems, recv_sems, 0)
    y_val = (base[...].astype(F32) + total).astype(BF16)
    y_ref[...] = y_val
    contract = (((1,), (1 if transpose else 0,)), ((), ()))
    mixed = lax.dot_general(y_val, w_mix[...], contract, preferred_element_type=F32)
    next_ref[...] = (y_val.astype(F32) + mixed).astype(BF16)
    if want_all:
        line_gather(next_ref, all_ref, send_sems, recv_sems, N_RS)


def pass_line(part, base, w_mix, transpose, want_all, collective_id):
    _, tok, width = part.shape
    block = jax.ShapeDtypeStruct((tok, width), BF16)
    outs = [block, block] + ([jax.ShapeDtypeStruct((8, tok, width), BF16)] if want_all else [])
    n_sem = N_RS + (N_AG if want_all else 0)
    return pl.pallas_call(
        functools.partial(pass_kernel, transpose, want_all), name='pass_line',
        out_shape=outs, in_specs=[VMEM] * 3, out_specs=[VMEM] * len(outs),
        scratch_shapes=reduce_scratch(tok, width) + [pltpu.SemaphoreType.DMA((n_sem,)),
                                                     pltpu.SemaphoreType.DMA((n_sem,))],
        compiler_params=params(collective_id))(part, base, w_mix)


def mix_peers():
    at = {axis: lax.axis_index(axis) for axis in 'xyz'}
    return at, {axis: [{axis: lax.rem(at[axis] + k, 4)} for k in (1, 2, 3)] for axis in 'xyz'}


def mix_steps(grad, out, bufs, send_sems, recv_sems, base):
    dp = lax.axis_index('dp')
    mate = {'dp': 1 - dp}
    at, peers = mix_peers()
    mate_in, quarter_in, block, y_in, y_out, z_in, z_out = bufs
    quarter = grad.shape[1] // 4
    go = functools.partial(send, send_sems=send_sems, recv_sems=recv_sems)
    copies = []
    swap = go(grad.at[1 - dp], mate_in, index=base, peer=mate)
    yield
    swap.wait_recv()
    block[...] = (grad[dp].astype(F32) + mate_in[...].astype(F32)).astype(BF16)
    mine = pl.ds(pl.multiple_of(at['x'] * quarter, quarter), quarter)
    stage = []
    for k in range(3):
        rows = pl.ds(pl.multiple_of(lax.rem(at['x'] + k + 1, 4) * quarter, quarter), quarter)
        stage.append(go(block.at[rows], quarter_in.at[k], index=base + 1 + k, peer=peers['x'][k]))
    copies += [swap] + stage
    yield
    total = block[mine].astype(F32)
    for k in range(3):
        stage[k].wait_recv()
        total = total + quarter_in[k].astype(F32)
    for axis, buf_in, buf_out, first in (('y', y_in, y_out, base + 4), ('z', z_in, z_out, base + 7)):
        buf_out[...] = total.astype(BF16)
        stage = [go(buf_out, buf_in.at[k], index=first + k, peer=peers[axis][k]) for k in range(3)]
        copies += stage
        terms = [buf_out[...].astype(F32)]
        for k in range(3):
            stage[k].wait_recv()
            terms.append(buf_in[k].astype(F32))
        here = at[axis]
        total = None
        for coord in range(4):
            term = jnp.zeros_like(terms[0])
            for k in range(4):
                source = lax.rem(here + 4 - k, 4)
                term = jnp.where(source == coord, terms[k], term)
            total = term if total is None else total + term
    final = total.astype(BF16)
    out[dp, mine] = final
    stage = [go(out.at[dp, mine], out.at[dp, mine], index=base + 10 + k, peer=peers['x'][k]) for k in range(3)]
    copies += stage
    for k in range(3):
        stage[k].wait_recv()
    swap = go(out.at[dp], out.at[dp], index=base + 13, peer=mate)
    swap.wait_recv()
    copies.append(swap)
    for copy in copies:
        copy.wait_send()
    yield


N_MIX = 14


def close_kernel(part_v, base_v, w_mix, x_in, mix_top, part_y, base_y, dx_ref, y_ref, mix_ref, *scratch):
    bufs_v, bufs_y, bufs_m = scratch[:6], scratch[6:12], scratch[12:19]
    grad, send_sems, recv_sems = scratch[19:]
    _, _, _, _, mate = line_peers()
    _, peers = mix_peers()
    enter(peers['x'] + peers['y'] + peers['z'] + [mate])
    steps_v = line_reduce_steps(part_v, bufs_v, send_sems, recv_sems, 0)
    steps_y = line_reduce_steps(part_y, bufs_y, send_sems, recv_sems, N_RS)
    steps_m = mix_steps(grad, mix_ref, bufs_m, send_sems, recv_sems, 2 * N_RS)
    next(steps_v)
    next(steps_y)
    grad[1] = mix_top[...]
    next(steps_v)
    d_u = (base_v[...].astype(F32) + next(steps_v)).astype(BF16)
    grad[0] = tn(x_in[...], d_u).astype(BF16)
    next(steps_m)
    dx_ref[...] = (d_u.astype(F32) + nt(d_u, w_mix[...])).astype(BF16)
    next(steps_m)
    next(steps_y)
    next(steps_m)
    y_ref[...] = (base_y[...].astype(F32) + next(steps_y)).astype(BF16)


def close_line(part_v, base_v, w_mix, x_in, mix_top, part_y, base_y, collective_id):
    _, tok, width = part_v.shape
    quarter = width // 4
    n_sem = 2 * N_RS + N_MIX
    block = jax.ShapeDtypeStruct((tok, width), BF16)
    return pl.pallas_call(
        close_kernel, name='close_line',
        out_shape=[block, block, jax.ShapeDtypeStruct((2, width, width), BF16)],
        in_specs=[VMEM] * 7, out_specs=[VMEM] * 3,
        scratch_shapes=reduce_scratch(tok, width) * 2
        + [pltpu.VMEM((width, width), BF16), pltpu.VMEM((3, quarter, width), BF16), pltpu.VMEM((width, width), BF16)]
        + [pltpu.VMEM((3, quarter, width), BF16), pltpu.VMEM((quarter, width), BF16)] * 2
        + [pltpu.VMEM((2, width, width), BF16), pltpu.SemaphoreType.DMA((n_sem,)), pltpu.SemaphoreType.DMA((n_sem,))],
        compiler_params=params(collective_id))(part_v, base_v, w_mix, x_in, mix_top, part_y, base_y)


N_PLANE = 40


def plane_gather_steps(src, dst, send_sems, recv_sems, base):
    at = {axis: lax.axis_index(axis) for axis in 'xy'}
    rows = src.shape[2] // 2
    part = (pl.ds(0, rows), pl.ds(rows, rows))
    go = functools.partial(send, send_sems=send_sems, recv_sems=recv_sems)
    copies = []

    def block(half, i, j):
        dx, dy = (i, j) if half == 0 else (j, i)
        return lax.rem(at['y'] + dy + 4, 4) * 4 + lax.rem(at['x'] + dx + 4, 4)

    def peer(half, stage, step):
        axis = 'xy'[stage] if half == 0 else 'yx'[stage]
        return {axis: lax.rem(at[axis] + step + 4, 4)}

    counter = [base]

    def launch(half, stage, step, i, j, rows_of=None, own=False):
        b = block(half, i, j)
        to = dst.at[b, :, half] if rows_of is None else dst.at[b, :, half, part[rows_of]]
        copy = go(src.at[:, half] if own else to, to, index=counter[0], peer=peer(half, stage, step))
        counter[0] += 1
        copies.append(copy)
        return copy

    first, second, relay1, relay2 = {}, {}, {}, {}
    for half in (0, 1):
        for step in (1, -1):
            first[half, step] = launch(half, 0, step, 0, 0, own=True)
    for half in (0, 1):
        for step in (1, -1):
            second[half, 0, step] = launch(half, 1, step, 0, 0, own=True)
    dst[at['y'] * 4 + at['x']] = src[...]
    yield
    for step in (1, -1):
        for half in (0, 1):
            first[half, step].wait_recv()
            relay1[half, step] = launch(half, 0, step, -step, 0, rows_of=0 if step == 1 else 1)
            for out in (1, -1):
                second[half, -step, out] = launch(half, 1, out, -step, 0)
    yield

    def forward(i):
        for step in (1, -1):
            for half in (0, 1):
                second[half, i, step].wait_recv()
                relay2[half, i, step] = launch(half, 1, step, i, -step, rows_of=0 if step == 1 else 1)

    forward(0)
    for half in (0, 1):
        for step in (1, -1):
            relay1[half, step].wait_recv()
        for out in (1, -1):
            second[half, 2, out] = launch(half, 1, out, 2, 0)
    yield
    forward(-1)
    forward(1)
    forward(2)
    for copy in relay2.values():
        copy.wait_recv()
    for copy in copies:
        copy.wait_send()
    yield


def open_kernel(n_chip, tok_src, route_src, w_src, tok_all, route, w_all, route_all, send_sems, recv_sems):
    z, dp, up, down, mate = line_peers()
    at = {axis: lax.axis_index(axis) for axis in 'xy'}
    enter([up, down, mate] + [{axis: lax.rem(at[axis] + k, 4)} for axis in 'xy' for k in (1, 3)])
    steps_w = plane_gather_steps(w_src, w_all, send_sems, recv_sems, 0)
    steps_r = line_gather_steps(route_src, route_all, send_sems, recv_sems, N_PLANE)
    steps_t = line_gather_steps(tok_src, tok_all, send_sems, recv_sems, N_PLANE + N_AG)
    next(steps_w)
    next(steps_r)
    next(steps_t)
    for steps in (steps_r, steps_w, steps_t):
        next(steps)
    next(steps_w)
    for steps in (steps_r, steps_t):
        for _ in steps:
            pass
    n_layers, _, _, n_mine, n_tok = route.shape
    n_half = n_chip // 2
    loc = lax.broadcasted_iota(jnp.int32, (n_mine, n_tok), 0)
    mine = ((z * 16 + loc // n_half) * n_chip + dp * n_half + lax.rem(loc, n_half)).astype(F32)
    row = lax.broadcasted_iota(jnp.int32, (n_tok, n_tok), 0)
    col = lax.broadcasted_iota(jnp.int32, (n_tok, n_tok), 1)
    before = jnp.where(row < col, 1.0, 0.0).astype(BF16)
    top_k = route_src.shape[0] // (4 * n_layers)
    for layer in range(n_layers):
        for s in range(8):
            rows = route_all[s, layer * 4 * top_k:(layer + 1) * 4 * top_k, :].astype(F32)
            used = jnp.zeros((n_mine, n_tok), F32)
            gates = [jnp.zeros((n_mine, n_tok), F32) for _ in range(3)]
            for j in range(top_k):
                hit = jnp.broadcast_to(rows[j:j + 1], mine.shape) == mine
                used = jnp.where(hit, 1.0, used)
                for k in range(3):
                    val = rows[(k + 1) * top_k + j:(k + 1) * top_k + j + 1]
                    gates[k] = jnp.where(hit, jnp.broadcast_to(val, mine.shape), gates[k])
            pos = nn(used.astype(BF16), before)
            route[layer, 0, s] = jnp.where(used > 0.5, pos, -1.0)
            for k in range(3):
                route[layer, 1 + k, s] = gates[k]
    for _ in steps_w:
        pass


def open_line(tok_src, route_src, w_src, n_layers, n_chip, collective_id):
    n_tok = route_src.shape[1]
    n_mine = 16 * n_chip // 2
    n_sem = N_PLANE + 2 * N_AG
    return pl.pallas_call(
        functools.partial(open_kernel, n_chip), name='open_line',
        out_shape=[jax.ShapeDtypeStruct((8,) + tok_src.shape, BF16),
                   jax.ShapeDtypeStruct((n_layers, 4, 8, n_mine, n_tok), F32),
                   jax.ShapeDtypeStruct((16,) + w_src.shape, BF16)],
        in_specs=[VMEM] * 3, out_specs=[VMEM] * 3,
        scratch_shapes=[pltpu.VMEM((8,) + route_src.shape, BF16),
                        pltpu.SemaphoreType.DMA((n_sem,)), pltpu.SemaphoreType.DMA((n_sem,))],
        compiler_params=params(collective_id))(tok_src, route_src, w_src)


def silu_parts(pre_gate):
    sig_val = jax.nn.sigmoid(pre_gate)
    return pre_gate * sig_val, sig_val * (1.0 + pre_gate * (1.0 - sig_val))


def split3(val):
    hi = lax.reduce_precision(val, 8, 7)
    rest = val - hi
    mid = lax.reduce_precision(rest, 8, 7)
    return hi, mid, rest - mid


def dot(spec, a, b):
    return jnp.einsum(spec, a, b, preferred_element_type=F32)


CHUNK = 8
SLOT = 24
ROWS = 8 * SLOT


def one_hot(pos, source, values=None):
    n_experts, n_tok = pos.shape[1:]
    slots = lax.broadcasted_iota(jnp.int32, (SLOT, n_tok), 0).astype(F32)
    blocks = []
    for e in range(n_experts):
        mask = jnp.broadcast_to(pos[source, e:e + 1, :], slots.shape) == slots
        val = 1.0 if values is None else jnp.broadcast_to(values[e:e + 1], slots.shape)
        blocks.append(jnp.where(mask, val, 0.0))
    return jnp.concatenate(blocks, axis=0)


def nn(a, b):
    return lax.dot_general(a, b, (((1,), (0,)), ((), ())), preferred_element_type=F32)


def nt(a, b):
    return lax.dot_general(a, b, (((1,), (1,)), ((), ())), preferred_element_type=F32)


def tn(a, b):
    return lax.dot_general(a, b, (((0,), (0,)), ((), ())), preferred_element_type=F32)


def select_rows(rows_of, out):
    for pair in range(4):
        both = [rows_of(2 * pair), rows_of(2 * pair + 1)]
        for e in range(CHUNK):
            val = jnp.concatenate([rows[e * SLOT:(e + 1) * SLOT] for rows in both], axis=0)
            out[e, pair * 2 * SLOT:(pair + 1) * 2 * SLOT, :] = val.astype(BF16)


def select_tokens(pos, u_all, recv):
    select_rows(lambda s: nn(one_hot(pos, s).astype(BF16), u_all[s]), recv)


def select_grads(pos, hi, mid, lo, dy_all, grad_in):
    def rows_of(s):
        gate_slot = jnp.sum(one_hot(pos, s, (hi[s] + mid[s]) + lo[s]), axis=1, keepdims=True)
        return gate_slot * nn(one_hot(pos, s).astype(BF16), dy_all[s])

    select_rows(rows_of, grad_in)


def hidden_of(rows, w_in, e):
    both = nn(rows, jnp.concatenate([w_in[e // 2, 0, e % 2], w_in[e // 2, 1, e % 2]], axis=1))
    ff = both.shape[1] // 2
    a, b = both[:, :ff], both[:, ff:]
    act, _ = silu_parts(a)
    return a, b, (act * b).astype(BF16)


def expert_grads(c, rows, a, b, h, w_down, e, pack, d_gate, d_up):
    d_hidden = nn(c, w_down)
    act, slope = silu_parts(a)
    da = (d_hidden * b * slope).astype(BF16)
    db = (d_hidden * act).astype(BF16)
    d_gate[e] = da
    d_up[e] = db
    both = tn(rows, jnp.concatenate([da, db], axis=1)).astype(BF16)
    ff = both.shape[1] // 2
    pack[e // 2, 0, e % 2] = both[:, :ff]
    pack[e // 2, 1, e % 2] = both[:, ff:]
    pack[e // 2, 2, e % 2] = tn(c, h).astype(BF16)


def forward_kernel(pos, u_all, w_in, recv, pre_gate, pre_up, hidden):
    select_tokens(pos, u_all, recv)
    for e in range(CHUNK):
        pre_gate[e], pre_up[e], hidden[e] = hidden_of(recv[e], w_in, e)


def backward_kernel(pos, hi, mid, lo, dy_all, w_out, recv, pre_gate, pre_up, hidden, pack, d_gate, d_up, grad_in):
    select_grads(pos, hi, mid, lo, dy_all, grad_in)
    for e in range(CHUNK):
        expert_grads(grad_in[e], recv[e], pre_gate[e], pre_up[e], hidden[e], w_out[e // 2, 0, e % 2], e,
                     pack, d_gate, d_up)


def select_kernel(pos, hi, mid, lo, u_all, dy_all, recv, grad_in):
    select_tokens(pos, u_all, recv)
    select_grads(pos, hi, mid, lo, dy_all, grad_in)


def top_kernel(recv, grad_in, w_all, pack, d_gate, d_up, hidden):
    for e in range(CHUNK):
        rows = recv[e]
        a, b, h = hidden_of(rows, w_all, e)
        hidden[e] = h
        expert_grads(grad_in[e], rows, a, b, h, w_all[e // 2, 2, e % 2], e, pack, d_gate, d_up)


def combine_kernel(n_left, pos, hi, mid, lo, *refs):
    lefts, w_out, part, rows = refs[:n_left], refs[n_left], refs[n_left + 1], refs[n_left + 2]
    step = pl.program_id(0)
    for e in range(CHUNK):
        left = jnp.concatenate([ref[e] for ref in lefts], axis=1)
        right = jnp.concatenate([w_out[e // 2, k, e % 2] for k in range(n_left)], axis=1)
        rows[step * CHUNK + e] = nt(left, right).astype(BF16).astype(F32)

    @pl.when(step == pl.num_programs(0) - 1)
    def _():
        def source(s, carry):
            slots = pl.ds(pl.multiple_of(s * SLOT, 8), SLOT)
            mine = jnp.concatenate([rows[e, slots, :] for e in range(rows.shape[0])], axis=0).astype(BF16)
            val = tn(one_hot(pos, s, lo[s]).astype(BF16), mine)
            val = val + tn(one_hot(pos, s, mid[s]).astype(BF16), mine)
            part[s] = val + tn(one_hot(pos, s, hi[s]).astype(BF16), mine)
            return carry

        lax.fori_loop(0, 8, source, 0)


def route_specs(route, layer, kinds, n_experts=CHUNK):
    pick = (lambda i: i) if n_experts == CHUNK else (lambda i: 0)
    return [pl.BlockSpec((None, None, 8, n_experts, route.shape[4]), lambda i, k=k: (layer, k, 0, pick(i), 0))
            for k in kinds]


def token_spec(tok_all, n_tok, part):
    return pl.BlockSpec((8, n_tok, tok_all.shape[2]), lambda i: (0, part, 0))


def per_expert(last):
    return pl.BlockSpec((CHUNK, ROWS, last), lambda i: (i, 0, 0))


def weight_spec(weights, kinds, first):
    return pl.BlockSpec((CHUNK // 2, kinds, 2) + weights.shape[3:], lambda i: (i, first // kinds, 0, 0, 0))


def local_call(kernel, n_mine, outs, in_specs, out_specs, scratch=()):
    return pl.pallas_call(
        kernel, grid=(n_mine // CHUNK,), out_shape=outs, in_specs=in_specs, out_specs=out_specs,
        scratch_shapes=list(scratch), compiler_params=pltpu.CompilerParams(vmem_limit_bytes=60 * 1024 * 1024))


def per_slot(n_mine, last, dtype):
    return jax.ShapeDtypeStruct((n_mine, ROWS, last), dtype)


def expert_forward(route, layer, u_all, weights):
    n_mine, n_tok = route.shape[3:]
    width, ff = weights.shape[3:]
    return local_call(
        forward_kernel, n_mine,
        [per_slot(n_mine, width, BF16), per_slot(n_mine, ff, F32), per_slot(n_mine, ff, F32), per_slot(n_mine, ff, BF16)],
        route_specs(route, layer, (0,)) + [token_spec(u_all, n_tok, 0), weight_spec(weights, 2, 0)],
        [per_expert(width), per_expert(ff), per_expert(ff), per_expert(ff)])(route, u_all, weights)


def expert_backward(route, layer, dy_all, weights, recv, pre_gate, pre_up, hidden):
    n_mine, n_tok = route.shape[3:]
    width, ff = weights.shape[3:]
    return local_call(
        backward_kernel, n_mine,
        [jax.ShapeDtypeStruct(weights.shape, BF16), per_slot(n_mine, ff, BF16), per_slot(n_mine, ff, BF16)],
        route_specs(route, layer, (0, 1, 2, 3)) + [token_spec(dy_all, n_tok, 0), weight_spec(weights, 1, 2),
                                                   per_expert(width), per_expert(ff), per_expert(ff), per_expert(ff)],
        [weight_spec(weights, 3, 0), per_expert(ff), per_expert(ff)],
        [pltpu.VMEM((CHUNK, ROWS, width), BF16)])(*[route] * 4, dy_all, weights, recv, pre_gate, pre_up, hidden)


def expert_select(route, layer, u_all, dy_all, dy_part):
    n_mine, n_tok = route.shape[3:]
    width = u_all.shape[2]
    return local_call(
        select_kernel, n_mine, [per_slot(n_mine, width, BF16)] * 2,
        route_specs(route, layer, (0, 1, 2, 3)) + [token_spec(u_all, n_tok, 0), token_spec(dy_all, n_tok, dy_part)],
        [per_expert(width)] * 2)(*[route] * 4, u_all, dy_all)


def expert_top(recv, grad_in, weights):
    n_mine = recv.shape[0]
    width, ff = weights.shape[3:]
    return local_call(
        top_kernel, n_mine,
        [jax.ShapeDtypeStruct(weights.shape, BF16)] + [per_slot(n_mine, ff, BF16)] * 3,
        [per_expert(width)] * 2 + [weight_spec(weights, 3, 0)],
        [weight_spec(weights, 3, 0)] + [per_expert(ff)] * 3)(recv, grad_in, weights)


def expert_combine(route, layer, lefts, weights, which):
    n_mine, n_tok = route.shape[3:]
    width, ff = weights.shape[3:]
    return local_call(
        functools.partial(combine_kernel, len(lefts)), n_mine,
        jax.ShapeDtypeStruct((8, n_tok, width), F32),
        route_specs(route, layer, (0, 1, 2, 3), n_mine) + [per_expert(ff)] * len(lefts)
        + [weight_spec(weights, len(lefts), which)],
        pl.BlockSpec((8, n_tok, width), lambda i: (0, 0, 0)),
        [pltpu.VMEM((n_mine, ROWS, width), F32)])(*[route] * 4, *lefts, weights)


def solution(mesh):
    m4 = Mesh(mesh.devices.reshape(4, 4, 4, 2), ('z', 'y', 'x', 'dp'))
    ep = ('z', 'y', 'x')
    tok_spec = P(('dp',) + ep, None)
    route_spec = P(None, ('dp',) + ep, None)
    whole_spec = P(None, None, None)
    expert_spec = P(None, ep, None, None)

    def device_body(tokens, d_out, expert_ids, gate_vals, w_mix, w_gate, w_up, w_down):
        n_layers = w_mix.shape[0]
        n_chip = w_gate.shape[1]
        n_half = n_chip // 2
        _, d_model = tokens.shape
        ff = w_gate.shape[3]
        dp = lax.axis_index('dp')

        def own_weights(layer):
            wg = lax.dynamic_slice_in_dim(w_gate[layer], dp * n_half, n_half, 0)
            wu = lax.dynamic_slice_in_dim(w_up[layer], dp * n_half, n_half, 0)
            wd = lax.dynamic_slice_in_dim(w_down[layer], dp * n_half, n_half, 0)
            return jnp.stack([wg, wu, jnp.swapaxes(wd, 1, 2)], axis=0)

        def scatter_grads(pack):
            part = lax.psum_scatter(pack.reshape(16 * 3 * n_half * d_model, ff), ('y', 'x'),
                                    scatter_dimension=0, tiled=True)
            return part

        def finish_grads(part):
            other = lax.ppermute(part, 'dp', [(0, 1), (1, 0)])
            lo = jnp.where(dp == 0, part, other).reshape(3, n_half, d_model, ff)
            hi = jnp.where(dp == 0, other, part).reshape(3, n_half, d_model, ff)
            both = jnp.concatenate([lo, hi], axis=1)
            return both[0], both[1], jnp.swapaxes(both[2], 1, 2)

        route_src = []
        for layer in range(n_layers):
            route_src.append(expert_ids[layer].astype(BF16))
            route_src.extend(part.astype(BF16) for part in split3(gate_vals[layer]))
        route_src = jnp.concatenate(route_src, axis=1).T

        u_act = (tokens.astype(F32) + dot('td,de->te', tokens, w_mix[0])).astype(BF16)
        first = jnp.concatenate([u_act, d_out], axis=0)
        tok_all, route, w_first = open_line(first, route_src, own_weights(0), n_layers, n_chip, 1)
        own_top, w_first = lax.optimization_barrier((own_weights(1), w_first))
        w_top = lax.all_gather(own_top.reshape(3 * n_half * d_model, ff), ('y', 'x'), axis=0, tiled=False)
        w_top = w_top.reshape(16, 3, n_half, d_model, ff)

        low = expert_forward(route, 0, tok_all, w_first)
        part = expert_combine(route, 0, low[3:], w_first, 2)
        y_low, u_top, u_all = pass_line(part, u_act, w_mix[1], False, True, 2)

        recv, grad_in = expert_select(route, 1, u_all, tok_all, 1)
        w_top, recv = lax.optimization_barrier((w_top, recv))
        pack, d_gate, d_up, hidden = expert_top(recv, grad_in, w_top)
        grad_top = scatter_grads(pack)
        part = expert_combine(route, 1, (d_gate, d_up), w_top, 0)
        d_u, d_y, dy_all = pass_line(part, d_out, w_mix[1], True, True, 3)
        mix_top = dot('td,te->de', y_low, d_u).astype(BF16)

        pack, d_gate, d_up = expert_backward(route, 0, dy_all, w_first, *low)
        grad_low = scatter_grads(pack)
        part_v = expert_combine(route, 0, (d_gate, d_up), w_first, 0)
        hidden, part_v = lax.optimization_barrier((hidden, part_v))
        part_y = expert_combine(route, 1, (hidden,), w_top, 2)
        d_tokens, layer_out, mix_out = close_line(part_v, d_y, w_mix[0], tokens, mix_top, part_y, u_top, 4)
        grad_top, d_tokens = lax.optimization_barrier((grad_top, d_tokens))
        grads = [finish_grads(grad_low), finish_grads(grad_top)]
        return (layer_out, d_tokens, mix_out) + tuple(jnp.stack([g[k] for g in grads]) for k in range(3))

    return jax.shard_map(device_body, mesh=m4,
                         in_specs=(tok_spec, tok_spec, route_spec, route_spec, whole_spec,
                                   expert_spec, expert_spec, expert_spec),
                         out_specs=(tok_spec, tok_spec, whole_spec, expert_spec, expert_spec, expert_spec),
                         check_vma=False)
```

```python
import functools
import jax
import jax.numpy as jnp
from jax import lax
from jax.experimental import pallas as pl
from jax.experimental.pallas import tpu as pltpu
from jax.sharding import Mesh, PartitionSpec as P


F32 = jnp.float32
BF16 = jnp.bfloat16
MESH = pl.DeviceIdType.MESH
VMEM = pl.BlockSpec(memory_space=pltpu.VMEM)


def ring(at, step):
    return lax.rem(at + (step + 4), 4)


def enter(peers):
    barrier = pltpu.get_barrier_semaphore()
    for peer in peers:
        pl.semaphore_signal(barrier, inc=1, device_id=peer, device_id_type=MESH)
    pl.semaphore_wait(barrier, len(peers))


def send(src, dst, send_sems, recv_sems, index, peer):
    copy = pltpu.make_async_remote_copy(src_ref=src, dst_ref=dst, send_sem=send_sems.at[index],
                                        recv_sem=recv_sems.at[index], device_id=peer, device_id_type=MESH)
    copy.start()
    return copy


def line_peers():
    z, dp = lax.axis_index('z'), lax.axis_index('dp')
    up, down = {'z': ring(z, 1)}, {'z': ring(z, -1)}
    return z, dp, up, down, {'dp': 1 - dp}


N_AG = 9


def line_gather(src, dst, send_sems, recv_sems, base):
    for _ in line_gather_steps(src, dst, send_sems, recv_sems, base):
        pass


def line_gather_steps(src, dst, send_sems, recv_sems, base):
    z, dp, up, down, mate = line_peers()
    rows = src.shape[0]
    half = rows // 2
    me = z * 2 + dp
    below, above, far = [ring(z, step) * 2 + dp for step in (-1, 1, 2)]
    lo, hi = pl.ds(0, half), pl.ds(half, half)
    go = functools.partial(send, send_sems=send_sems, recv_sems=recv_sems)
    to_up = go(src, dst.at[me], index=base, peer=up)
    to_down = go(src, dst.at[me], index=base + 1, peer=down)
    to_mate = go(src, dst.at[me], index=base + 2, peer=mate)
    dst[me] = src[...]
    yield
    to_up.wait_recv()
    relay_up = go(dst.at[below, lo], dst.at[below, lo], index=base + 3, peer=up)
    mate_below = go(dst.at[below], dst.at[below], index=base + 5, peer=mate)
    to_down.wait_recv()
    relay_down = go(dst.at[above, hi], dst.at[above, hi], index=base + 4, peer=down)
    mate_above = go(dst.at[above], dst.at[above], index=base + 6, peer=mate)
    yield
    relay_up.wait_recv()
    mate_lo = go(dst.at[far, lo], dst.at[far, lo], index=base + 7, peer=mate)
    relay_down.wait_recv()
    mate_hi = go(dst.at[far, hi], dst.at[far, hi], index=base + 8, peer=mate)
    for copy in (to_mate, mate_below, mate_above, mate_lo, mate_hi):
        copy.wait_recv()
    for copy in (to_up, to_down, to_mate, relay_up, relay_down, mate_below, mate_above, mate_lo, mate_hi):
        copy.wait_send()


N_RS = 10


def line_reduce_steps(part, bufs, send_sems, recv_sems, base):
    d_part, sums, relay_lo, relay_hi, in_lo, in_hi = bufs
    z, dp, up, down, mate = line_peers()
    half = part.shape[1] // 2
    lo, hi = pl.ds(0, half), pl.ds(half, half)
    order = [ring(z, step) for step in (2, 1, -1, 0)]
    go = functools.partial(send, send_sems=send_sems, recv_sems=recv_sems)
    swaps = [go(part.at[zk * 2 + 1 - dp], d_part.at[k], index=base + k, peer=mate) for k, zk in enumerate(order)]
    yield
    swaps[0].wait_recv()
    sums[0] = part[order[0] * 2 + dp] + d_part[0]
    far_up = go(sums.at[0, lo], relay_lo, index=base + 4, peer=up)
    far_down = go(sums.at[0, hi], relay_hi, index=base + 5, peer=down)
    swaps[1].wait_recv()
    sums[1] = part[order[1] * 2 + dp] + d_part[1]
    up_hi = go(sums.at[1, hi], in_lo.at[hi], index=base + 6, peer=up)
    swaps[2].wait_recv()
    sums[2] = part[order[2] * 2 + dp] + d_part[2]
    down_lo = go(sums.at[2, lo], in_hi.at[lo], index=base + 7, peer=down)
    swaps[3].wait_recv()
    sums[3] = part[order[3] * 2 + dp] + d_part[3]
    far_up.wait_recv()
    sums[1, lo] = sums[1, lo] + relay_lo[...]
    up_lo = go(sums.at[1, lo], in_lo.at[lo], index=base + 8, peer=up)
    far_down.wait_recv()
    sums[2, hi] = sums[2, hi] + relay_hi[...]
    down_hi = go(sums.at[2, hi], in_hi.at[hi], index=base + 9, peer=down)
    yield
    for copy in (up_hi, down_lo, up_lo, down_hi):
        copy.wait_recv()
    for copy in swaps + [far_up, far_down, up_hi, down_lo, up_lo, down_hi]:
        copy.wait_send()
    yield sums[3] + in_lo[...] + in_hi[...]


def line_reduce(part, bufs, send_sems, recv_sems, base):
    for total in line_reduce_steps(part, bufs, send_sems, recv_sems, base):
        pass
    return total


def reduce_scratch(tok, width):
    return [pltpu.VMEM((4, tok, width), F32), pltpu.VMEM((4, tok, width), F32),
            pltpu.VMEM((tok // 2, width), F32), pltpu.VMEM((tok // 2, width), F32),
            pltpu.VMEM((tok, width), F32), pltpu.VMEM((tok, width), F32)]


def params(collective_id):
    return pltpu.CompilerParams(collective_id=collective_id, has_side_effects=True,
                                vmem_limit_bytes=60 * 1024 * 1024)


def pass_kernel(transpose, want_all, part, base, w_mix, y_ref, next_ref, *rest):
    if want_all:
        all_ref, rest = rest[0], rest[1:]
    bufs, (send_sems, recv_sems) = rest[:-2], rest[-2:]
    _, _, up, down, mate = line_peers()
    enter((up, down, mate))
    total = line_reduce(part, bufs, send_sems, recv_sems, 0)
    y_val = (base[...].astype(F32) + total).astype(BF16)
    y_ref[...] = y_val
    contract = (((1,), (1 if transpose else 0,)), ((), ()))
    mixed = lax.dot_general(y_val, w_mix[...], contract, preferred_element_type=F32)
    next_ref[...] = (y_val.astype(F32) + mixed).astype(BF16)
    if want_all:
        line_gather(next_ref, all_ref, send_sems, recv_sems, N_RS)


def pass_line(part, base, w_mix, transpose, want_all, collective_id):
    _, tok, width = part.shape
    block = jax.ShapeDtypeStruct((tok, width), BF16)
    outs = [block, block] + ([jax.ShapeDtypeStruct((8, tok, width), BF16)] if want_all else [])
    n_sem = N_RS + (N_AG if want_all else 0)
    return pl.pallas_call(
        functools.partial(pass_kernel, transpose, want_all), name='pass_line',
        out_shape=outs, in_specs=[VMEM] * 3, out_specs=[VMEM] * len(outs),
        scratch_shapes=reduce_scratch(tok, width) + [pltpu.SemaphoreType.DMA((n_sem,)),
                                                     pltpu.SemaphoreType.DMA((n_sem,))],
        compiler_params=params(collective_id))(part, base, w_mix)


def mix_peers():
    at = {axis: lax.axis_index(axis) for axis in 'xyz'}
    return at, {axis: [{axis: ring(at[axis], k)} for k in (1, 2, 3)] for axis in 'xyz'}


def mix_steps(grad, out, bufs, send_sems, recv_sems, base):
    dp = lax.axis_index('dp')
    mate = {'dp': 1 - dp}
    at, peers = mix_peers()
    mate_in, quarter_in, block, y_in, y_out, z_in, z_out = bufs
    quarter = grad.shape[1] // 4
    go = functools.partial(send, send_sems=send_sems, recv_sems=recv_sems)
    copies = []
    swap = go(grad.at[1 - dp], mate_in, index=base, peer=mate)
    yield
    swap.wait_recv()
    block[...] = (grad[dp].astype(F32) + mate_in[...].astype(F32)).astype(BF16)
    mine = pl.ds(pl.multiple_of(at['x'] * quarter, quarter), quarter)
    stage = []
    for k in range(3):
        rows = pl.ds(pl.multiple_of(ring(at['x'], k + 1) * quarter, quarter), quarter)
        stage.append(go(block.at[rows], quarter_in.at[k], index=base + 1 + k, peer=peers['x'][k]))
    copies += [swap] + stage
    yield
    total = block[mine].astype(F32)
    for k in range(3):
        stage[k].wait_recv()
        total = total + quarter_in[k].astype(F32)
    for axis, buf_in, buf_out, first in (('y', y_in, y_out, base + 4), ('z', z_in, z_out, base + 7)):
        buf_out[...] = total.astype(BF16)
        stage = [go(buf_out, buf_in.at[k], index=first + k, peer=peers[axis][k]) for k in range(3)]
        copies += stage
        terms = [buf_out[...].astype(F32)]
        for k in range(3):
            stage[k].wait_recv()
            terms.append(buf_in[k].astype(F32))
        here = at[axis]
        total = None
        for coord in range(4):
            term = jnp.zeros_like(terms[0])
            for k in range(4):
                source = ring(here, -k)
                term = jnp.where(source == coord, terms[k], term)
            total = term if total is None else total + term
    final = total.astype(BF16)
    out[dp, mine] = final
    stage = [go(out.at[dp, mine], out.at[dp, mine], index=base + 10 + k, peer=peers['x'][k]) for k in range(3)]
    copies += stage
    for k in range(3):
        stage[k].wait_recv()
    swap = go(out.at[dp], out.at[dp], index=base + 13, peer=mate)
    swap.wait_recv()
    copies.append(swap)
    for copy in copies:
        copy.wait_send()
    yield


N_MIX = 14


def close_kernel(part_v, base_v, w_mix, x_in, mix_top, part_y, base_y, dx_ref, y_ref, mix_ref, *scratch):
    bufs_v, bufs_y, bufs_m = scratch[:6], scratch[6:12], scratch[12:19]
    grad, send_sems, recv_sems = scratch[19:]
    _, _, _, _, mate = line_peers()
    _, peers = mix_peers()
    enter(peers['x'] + peers['y'] + peers['z'] + [mate])
    steps_v = line_reduce_steps(part_v, bufs_v, send_sems, recv_sems, 0)
    steps_y = line_reduce_steps(part_y, bufs_y, send_sems, recv_sems, N_RS)
    steps_m = mix_steps(grad, mix_ref, bufs_m, send_sems, recv_sems, 2 * N_RS)
    next(steps_v)
    next(steps_y)
    grad[1] = mix_top[...]
    next(steps_v)
    d_u = (base_v[...].astype(F32) + next(steps_v)).astype(BF16)
    grad[0] = tn(x_in[...], d_u).astype(BF16)
    next(steps_m)
    dx_ref[...] = (d_u.astype(F32) + nt(d_u, w_mix[...])).astype(BF16)
    next(steps_m)
    next(steps_y)
    next(steps_m)
    y_ref[...] = (base_y[...].astype(F32) + next(steps_y)).astype(BF16)


def close_line(part_v, base_v, w_mix, x_in, mix_top, part_y, base_y, collective_id):
    _, tok, width = part_v.shape
    quarter = width // 4
    n_sem = 2 * N_RS + N_MIX
    block = jax.ShapeDtypeStruct((tok, width), BF16)
    return pl.pallas_call(
        close_kernel, name='close_line',
        out_shape=[block, block, jax.ShapeDtypeStruct((2, width, width), BF16)],
        in_specs=[VMEM] * 7, out_specs=[VMEM] * 3,
        scratch_shapes=reduce_scratch(tok, width) * 2
        + [pltpu.VMEM((width, width), BF16), pltpu.VMEM((3, quarter, width), BF16), pltpu.VMEM((width, width), BF16)]
        + [pltpu.VMEM((3, quarter, width), BF16), pltpu.VMEM((quarter, width), BF16)] * 2
        + [pltpu.VMEM((2, width, width), BF16), pltpu.SemaphoreType.DMA((n_sem,)), pltpu.SemaphoreType.DMA((n_sem,))],
        compiler_params=params(collective_id))(part_v, base_v, w_mix, x_in, mix_top, part_y, base_y)


N_PLANE = 40
WAYS = (1, -1)
HALVES = (0, 1)


def plane_gather_steps(src, dst, send_sems, recv_sems, base):
    at = {axis: lax.axis_index(axis) for axis in 'xy'}
    rows = src.shape[2] // 2
    part = (pl.ds(0, rows), pl.ds(rows, rows))
    go = functools.partial(send, send_sems=send_sems, recv_sems=recv_sems)
    copies = []

    def block(half, i, j):
        dx, dy = (i, j) if half == 0 else (j, i)
        return ring(at['y'], dy) * 4 + ring(at['x'], dx)

    def peer(half, stage, step):
        axis = 'xy'[stage] if half == 0 else 'yx'[stage]
        return {axis: ring(at[axis], step)}

    counter = [base]

    def launch(half, stage, step, i, j, rows_of=None, own=False):
        b = block(half, i, j)
        to = dst.at[b, :, half] if rows_of is None else dst.at[b, :, half, part[rows_of]]
        copy = go(src.at[:, half] if own else to, to, index=counter[0], peer=peer(half, stage, step))
        counter[0] += 1
        copies.append(copy)
        return copy

    first, second, relay1, relay2 = {}, {}, {}, {}
    for half in HALVES:
        for step in WAYS:
            first[half, step] = launch(half, 0, step, 0, 0, own=True)
    for half in HALVES:
        for step in WAYS:
            second[half, 0, step] = launch(half, 1, step, 0, 0, own=True)
    dst[at['y'] * 4 + at['x']] = src[...]
    yield
    for step in WAYS:
        for half in HALVES:
            first[half, step].wait_recv()
            relay1[half, step] = launch(half, 0, step, -step, 0, rows_of=0 if step == 1 else 1)
            for out in WAYS:
                second[half, -step, out] = launch(half, 1, out, -step, 0)
    yield

    def forward(i):
        for step in WAYS:
            for half in HALVES:
                second[half, i, step].wait_recv()
                relay2[half, i, step] = launch(half, 1, step, i, -step, rows_of=0 if step == 1 else 1)

    forward(0)
    for half in HALVES:
        for step in WAYS:
            relay1[half, step].wait_recv()
        for out in WAYS:
            second[half, 2, out] = launch(half, 1, out, 2, 0)
    yield
    forward(-1)
    forward(1)
    forward(2)
    for copy in relay2.values():
        copy.wait_recv()
    for copy in copies:
        copy.wait_send()
    yield


def open_kernel(n_chip, tokens, d_out, w_mix, ids, hi, mid, lo, w_gate, w_up, w_down,
                tok_all, route, w_all, w_top, u_ref,
                tok_src, route_src, w_src, route_all, load_sems, send_sems, recv_sems):
    z, dp, up, down_peer, mate = line_peers()
    at = {axis: lax.axis_index(axis) for axis in 'xy'}
    n_half = n_chip // 2
    own = pl.ds(dp * n_half, n_half)
    loads = []
    for layer, dst in enumerate((w_src, w_top)):
        for k, (src, to) in enumerate(((w_gate, dst.at[0]), (w_up, dst.at[1]), (w_down, dst.at[2]))):
            loads.append(pltpu.make_async_copy(src.at[layer, own], to, load_sems.at[layer, k]))
    for load in loads:
        load.start()
    enter([up, down_peer, mate] + [{axis: ring(at[axis], k)} for axis in 'xy' for k in WAYS])

    def unit(size):
        row = lax.broadcasted_iota(jnp.int32, (size, size), 0)
        col = lax.broadcasted_iota(jnp.int32, (size, size), 1)
        return jnp.where(row == col, 1.0, 0.0).astype(BF16)

    for load in loads[:3]:
        load.wait()
    steps_w = plane_gather_steps(w_src, w_all, send_sems, recv_sems, 0)
    steps_r = line_gather_steps(route_src, route_all, send_sems, recv_sems, N_PLANE)
    steps_t = line_gather_steps(tok_src, tok_all, send_sems, recv_sems, N_PLANE + N_AG)
    next(steps_w)
    width, tok = tokens.shape
    columns = [ref[layer] for layer in range(route.shape[0]) for ref in (ids, hi, mid, lo)]
    route_src[...] = jnp.concatenate(columns, axis=0).astype(BF16)
    next(steps_r)
    same = unit(width)
    u = (tn(tokens[...], same) + tn(tokens[...], w_mix[0])).astype(BF16)
    u_ref[...] = u
    tok_src[:tok] = u
    tok_src[tok:] = tn(d_out[...], same).astype(BF16)
    next(steps_t)
    for load in loads[3:]:
        load.wait()
    for steps in (steps_r, steps_w, steps_t):
        next(steps)
    next(steps_w)
    for steps in (steps_r, steps_t):
        for _ in steps:
            pass
    n_layers, _, _, n_mine, n_tok = route.shape
    loc = lax.broadcasted_iota(jnp.int32, (n_mine, n_tok), 0)
    mine = ((z * 16 + loc // n_half) * n_chip + dp * n_half + lax.rem(loc, n_half)).astype(F32)
    row = lax.broadcasted_iota(jnp.int32, (n_tok, n_tok), 0)
    col = lax.broadcasted_iota(jnp.int32, (n_tok, n_tok), 1)
    before = jnp.where(row < col, 1.0, 0.0).astype(BF16)
    top_k = route_src.shape[0] // (4 * n_layers)
    for layer in range(n_layers):
        for s in range(8):
            rows = route_all[s, layer * 4 * top_k:(layer + 1) * 4 * top_k, :].astype(F32)
            used = jnp.zeros((n_mine, n_tok), F32)
            gates = [jnp.zeros((n_mine, n_tok), F32) for _ in range(3)]
            for j in range(top_k):
                hit = jnp.broadcast_to(rows[j:j + 1], mine.shape) == mine
                used = jnp.where(hit, 1.0, used)
                for k in range(3):
                    val = rows[(k + 1) * top_k + j:(k + 1) * top_k + j + 1]
                    gates[k] = jnp.where(hit, jnp.broadcast_to(val, mine.shape), gates[k])
            pos = nn(used.astype(BF16), before)
            route[layer, 0, s] = jnp.where(used > 0.5, pos, -1.0)
            for k in range(3):
                route[layer, 1 + k, s] = gates[k]
    for _ in steps_w:
        pass


def open_line(tokens, d_out, w_mix, routing, w_gate, w_up, w_down, collective_id):
    width, tok = tokens.shape
    n_layers, n_chip, _, ff = w_gate.shape
    n_half = n_chip // 2
    n_rows = 4 * n_layers * routing[0].shape[1]
    n_sem = N_PLANE + 2 * N_AG
    own = (3, n_half, width, ff)
    anywhere = pl.BlockSpec(memory_space=pl.ANY)
    return pl.pallas_call(
        functools.partial(open_kernel, n_chip), name='open_line',
        out_shape=[jax.ShapeDtypeStruct((8, 2 * tok, width), BF16),
                   jax.ShapeDtypeStruct((n_layers, 4, 8, 16 * n_half, tok), F32),
                   jax.ShapeDtypeStruct((16,) + own, BF16), jax.ShapeDtypeStruct(own, BF16),
                   jax.ShapeDtypeStruct((tok, width), BF16)],
        in_specs=[VMEM] * 7 + [anywhere] * 3, out_specs=[VMEM] * 5,
        scratch_shapes=[pltpu.VMEM((2 * tok, width), BF16), pltpu.VMEM((n_rows, tok), BF16), pltpu.VMEM(own, BF16),
                        pltpu.VMEM((8, n_rows, tok), BF16),
                        pltpu.SemaphoreType.DMA((n_layers, 3)),
                        pltpu.SemaphoreType.DMA((n_sem,)), pltpu.SemaphoreType.DMA((n_sem,))],
        compiler_params=params(collective_id))(tokens, d_out, w_mix, *routing, w_gate, w_up, w_down)


def silu_parts(pre_gate):
    sig_val = jax.nn.sigmoid(pre_gate)
    return pre_gate * sig_val, sig_val * (1.0 + pre_gate * (1.0 - sig_val))


def split3(val):
    hi = lax.reduce_precision(val, 8, 7)
    rest = val - hi
    mid = lax.reduce_precision(rest, 8, 7)
    return hi, mid, rest - mid


def dot(spec, a, b):
    return jnp.einsum(spec, a, b, preferred_element_type=F32)


CHUNK = 8
TOP_CHUNK = 4
SLOT = 24
ROWS = 8 * SLOT


def one_hot(pos, source, values=None):
    n_experts, n_tok = pos.shape[1:]
    slots = lax.broadcasted_iota(jnp.int32, (SLOT, n_tok), 0).astype(F32)
    blocks = []
    for e in range(n_experts):
        mask = jnp.broadcast_to(pos[source, e:e + 1, :], slots.shape) == slots
        val = 1.0 if values is None else jnp.broadcast_to(values[e:e + 1], slots.shape)
        blocks.append(jnp.where(mask, val, 0.0))
    return jnp.concatenate(blocks, axis=0)


def nn(a, b):
    return lax.dot_general(a, b, (((1,), (0,)), ((), ())), preferred_element_type=F32)


def nt(a, b):
    return lax.dot_general(a, b, (((1,), (1,)), ((), ())), preferred_element_type=F32)


def tn(a, b):
    return lax.dot_general(a, b, (((0,), (0,)), ((), ())), preferred_element_type=F32)


def select_rows(rows_of, out):
    for pair in range(4):
        both = [rows_of(2 * pair), rows_of(2 * pair + 1)]
        for e in range(CHUNK):
            val = jnp.concatenate([rows[e * SLOT:(e + 1) * SLOT] for rows in both], axis=0)
            out[e, pair * 2 * SLOT:(pair + 1) * 2 * SLOT, :] = val.astype(BF16)


def select_tokens(pos, u_all, recv):
    select_rows(lambda s: nn(one_hot(pos, s).astype(BF16), u_all[s]), recv)


def select_grads(pos, hi, mid, lo, dy_all, grad_in):
    def rows_of(s):
        gate_slot = jnp.sum(one_hot(pos, s, (hi[s] + mid[s]) + lo[s]), axis=1, keepdims=True)
        return gate_slot * nn(one_hot(pos, s).astype(BF16), dy_all[s])

    select_rows(rows_of, grad_in)


def hidden_of(rows, w_in, e):
    both = nn(rows, jnp.concatenate([w_in[e // 2, 0, e % 2], w_in[e // 2, 1, e % 2]], axis=1))
    ff = both.shape[1] // 2
    a, b = both[:, :ff], both[:, ff:]
    act, _ = silu_parts(a)
    return a, b, (act * b).astype(BF16)


def expert_grads(c, rows, a, b, h, w_down, e, pack, d_gate, d_up):
    d_hidden = nn(c, w_down)
    act, slope = silu_parts(a)
    da = (d_hidden * b * slope).astype(BF16)
    db = (d_hidden * act).astype(BF16)
    d_gate[e] = da
    d_up[e] = db
    both = tn(rows, jnp.concatenate([da, db], axis=1)).astype(BF16)
    ff = both.shape[1] // 2
    pack[e // 2, 0, e % 2] = both[:, :ff]
    pack[e // 2, 1, e % 2] = both[:, ff:]
    pack[e // 2, 2, e % 2] = tn(c, h).astype(BF16)


def forward_kernel(pos, u_all, w_in, recv, pre_gate, pre_up, hidden):
    select_tokens(pos, u_all, recv)
    for e in range(CHUNK):
        pre_gate[e], pre_up[e], hidden[e] = hidden_of(recv[e], w_in, e)


def backward_kernel(pos, hi, mid, lo, dy_all, w_out, recv, pre_gate, pre_up, hidden, pack, d_gate, d_up, grad_in):
    select_grads(pos, hi, mid, lo, dy_all, grad_in)
    for e in range(CHUNK):
        expert_grads(grad_in[e], recv[e], pre_gate[e], pre_up[e], hidden[e], w_out[e // 2, 0, e % 2], e,
                     pack, d_gate, d_up)


def select_kernel(pos, hi, mid, lo, u_all, dy_all, recv, grad_in):
    select_tokens(pos, u_all, recv)
    select_grads(pos, hi, mid, lo, dy_all, grad_in)


def top_kernel(recv, grad_in, w_all, pack, d_gate, d_up, hidden):
    for e in range(TOP_CHUNK):
        rows = recv[e]
        a, b, h = hidden_of(rows, w_all, e)
        hidden[e] = h
        expert_grads(grad_in[e], rows, a, b, h, w_all[e // 2, 2, e % 2], e, pack, d_gate, d_up)


def combine_kernel(n_left, pos, hi, mid, lo, *refs):
    lefts, w_out, part, rows = refs[:n_left], refs[n_left], refs[n_left + 1], refs[n_left + 2]
    step = pl.program_id(0)
    for e in range(CHUNK):
        left = jnp.concatenate([ref[e] for ref in lefts], axis=1)
        right = jnp.concatenate([w_out[e // 2, k, e % 2] for k in range(n_left)], axis=1)
        rows[step * CHUNK + e] = nt(left, right).astype(BF16).astype(F32)

    @pl.when(step == pl.num_programs(0) - 1)
    def _():
        def source(s, carry):
            slots = pl.ds(pl.multiple_of(s * SLOT, 8), SLOT)
            mine = jnp.concatenate([rows[e, slots, :] for e in range(rows.shape[0])], axis=0).astype(BF16)
            val = tn(one_hot(pos, s, lo[s]).astype(BF16), mine)
            val = val + tn(one_hot(pos, s, mid[s]).astype(BF16), mine)
            part[s] = val + tn(one_hot(pos, s, hi[s]).astype(BF16), mine)
            return carry

        lax.fori_loop(0, 8, source, 0)


def route_specs(route, layer, kinds, n_experts=CHUNK):
    pick = (lambda i: i) if n_experts == CHUNK else (lambda i: 0)
    return [pl.BlockSpec((None, None, 8, n_experts, route.shape[4]), lambda i, k=k: (layer, k, 0, pick(i), 0))
            for k in kinds]


def token_spec(tok_all, n_tok, part):
    return pl.BlockSpec((8, n_tok, tok_all.shape[2]), lambda i: (0, part, 0))


def per_expert(last, chunk=CHUNK):
    return pl.BlockSpec((chunk, ROWS, last), lambda i: (i, 0, 0))


def weight_spec(weights, kinds, first, chunk=CHUNK):
    return pl.BlockSpec((chunk // 2, kinds, 2) + weights.shape[3:], lambda i: (i, first // kinds, 0, 0, 0))


def local_call(kernel, n_mine, outs, in_specs, out_specs, scratch=(), chunk=CHUNK):
    return pl.pallas_call(
        kernel, grid=(n_mine // chunk,), out_shape=outs, in_specs=in_specs, out_specs=out_specs,
        scratch_shapes=list(scratch), compiler_params=pltpu.CompilerParams(vmem_limit_bytes=60 * 1024 * 1024))


def per_slot(n_mine, last, dtype):
    return jax.ShapeDtypeStruct((n_mine, ROWS, last), dtype)


def expert_forward(route, layer, u_all, weights):
    n_mine, n_tok = route.shape[3:]
    width, ff = weights.shape[3:]
    return local_call(
        forward_kernel, n_mine,
        [per_slot(n_mine, width, BF16), per_slot(n_mine, ff, F32), per_slot(n_mine, ff, F32), per_slot(n_mine, ff, BF16)],
        route_specs(route, layer, (0,)) + [token_spec(u_all, n_tok, 0), weight_spec(weights, 2, 0)],
        [per_expert(width), per_expert(ff), per_expert(ff), per_expert(ff)])(route, u_all, weights)


def expert_backward(route, layer, dy_all, weights, recv, pre_gate, pre_up, hidden):
    n_mine, n_tok = route.shape[3:]
    width, ff = weights.shape[3:]
    return local_call(
        backward_kernel, n_mine,
        [jax.ShapeDtypeStruct(weights.shape, BF16), per_slot(n_mine, ff, BF16), per_slot(n_mine, ff, BF16)],
        route_specs(route, layer, range(4)) + [token_spec(dy_all, n_tok, 0), weight_spec(weights, 1, 2),
                                                   per_expert(width), per_expert(ff), per_expert(ff), per_expert(ff)],
        [weight_spec(weights, 3, 0), per_expert(ff), per_expert(ff)],
        [pltpu.VMEM((CHUNK, ROWS, width), BF16)])(*[route] * 4, dy_all, weights, recv, pre_gate, pre_up, hidden)


def expert_select(route, layer, u_all, dy_all, dy_part):
    n_mine, n_tok = route.shape[3:]
    width = u_all.shape[2]
    return local_call(
        select_kernel, n_mine, [per_slot(n_mine, width, BF16)] * 2,
        route_specs(route, layer, range(4)) + [token_spec(u_all, n_tok, 0), token_spec(dy_all, n_tok, dy_part)],
        [per_expert(width)] * 2)(*[route] * 4, u_all, dy_all)


def expert_top(recv, grad_in, weights):
    n_mine = recv.shape[0]
    width, ff = weights.shape[3:]
    return local_call(
        top_kernel, n_mine,
        [jax.ShapeDtypeStruct(weights.shape, BF16)] + [per_slot(n_mine, ff, BF16)] * 3,
        [per_expert(width, TOP_CHUNK)] * 2 + [weight_spec(weights, 3, 0, TOP_CHUNK)],
        [weight_spec(weights, 3, 0, TOP_CHUNK)] + [per_expert(ff, TOP_CHUNK)] * 3, chunk=TOP_CHUNK)(
            recv, grad_in, weights)


def expert_combine(route, layer, lefts, weights, which):
    n_mine, n_tok = route.shape[3:]
    width, ff = weights.shape[3:]
    return local_call(
        functools.partial(combine_kernel, len(lefts)), n_mine,
        jax.ShapeDtypeStruct((8, n_tok, width), F32),
        route_specs(route, layer, range(4), n_mine) + [per_expert(ff)] * len(lefts)
        + [weight_spec(weights, len(lefts), which)],
        pl.BlockSpec((8, n_tok, width), lambda i: (0, 0, 0)),
        [pltpu.VMEM((n_mine, ROWS, width), F32)])(*[route] * 4, *lefts, weights)


def solution(mesh):
    m4 = Mesh(mesh.devices.reshape(4, 4, 4, 2), ('z', 'y', 'x', 'dp'))
    ep = ('z', 'y', 'x')
    tok_spec = P(('dp',) + ep, None)
    route_spec = P(None, ('dp',) + ep, None)
    whole_spec = P(None, None, None)
    expert_spec = P(None, ep, None, None)

    def device_body(tokens, d_out, expert_ids, gate_vals, w_mix, w_gate, w_up, w_down):
        n_chip = w_gate.shape[1]
        n_half = n_chip // 2
        _, d_model = tokens.shape
        ff = w_gate.shape[3]
        dp = lax.axis_index('dp')

        def scatter_grads(pack):
            part = lax.psum_scatter(pack.reshape(16 * 3 * n_half * d_model, ff), ('y', 'x'),
                                    scatter_dimension=0, tiled=True)
            return part

        def finish_grads(part):
            other = lax.ppermute(part, 'dp', [(0, 1), (1, 0)])
            lo = jnp.where(dp == 0, part, other).reshape(3, n_half, d_model, ff)
            hi = jnp.where(dp == 0, other, part).reshape(3, n_half, d_model, ff)
            both = jnp.concatenate([lo, hi], axis=1)
            return both[0], both[1], jnp.swapaxes(both[2], 1, 2)

        routing = [jnp.swapaxes(expert_ids, 1, 2).astype(F32)] + list(split3(jnp.swapaxes(gate_vals, 1, 2)))
        tok_all, route, w_first, own_top, u_act = open_line(tokens.T, d_out.T, w_mix, routing, w_gate, w_up,
                                                            jnp.swapaxes(w_down, 2, 3), 1)
        w_top = lax.all_gather(own_top.reshape(3 * n_half * d_model, ff), ('y', 'x'), axis=0, tiled=False)
        w_top = w_top.reshape(16, 3, n_half, d_model, ff)

        low = expert_forward(route, 0, tok_all, w_first)
        part = expert_combine(route, 0, low[3:], w_first, 2)
        y_low, u_top, u_all = pass_line(part, u_act, w_mix[1], False, True, 2)

        recv, grad_in = expert_select(route, 1, u_all, tok_all, 1)
        w_top, recv = lax.optimization_barrier((w_top, recv))
        pack, d_gate, d_up, hidden = expert_top(recv, grad_in, w_top)
        grad_top = scatter_grads(pack)
        part = expert_combine(route, 1, (d_gate, d_up), w_top, 0)
        d_u, d_y, dy_all = pass_line(part, d_out, w_mix[1], True, True, 3)
        mix_top = dot('td,te->de', y_low, d_u).astype(BF16)

        pack, d_gate, d_up = expert_backward(route, 0, dy_all, w_first, *low)
        grad_low = scatter_grads(pack)
        part_v = expert_combine(route, 0, (d_gate, d_up), w_first, 0)
        hidden, part_v = lax.optimization_barrier((hidden, part_v))
        part_y = expert_combine(route, 1, (hidden,), w_top, 2)
        d_tokens, layer_out, mix_out = close_line(part_v, d_y, w_mix[0], tokens, mix_top, part_y, u_top, 4)
        grad_top, d_tokens = lax.optimization_barrier((grad_top, d_tokens))
        grads = [finish_grads(grad_low), finish_grads(grad_top)]
        return (layer_out, d_tokens, mix_out) + tuple(jnp.stack([g[k] for g in grads]) for k in range(3))

    return jax.shard_map(device_body, mesh=m4,
                         in_specs=(tok_spec, tok_spec, route_spec, route_spec, whole_spec,
                                   expert_spec, expert_spec, expert_spec),
                         out_specs=(tok_spec, tok_spec, whole_spec, expert_spec, expert_spec, expert_spec),
                         check_vma=False)
```

```python
import functools
import jax
import jax.numpy as jnp
from jax import lax
from jax.experimental import pallas as pl
from jax.experimental.pallas import tpu as pltpu
from jax.sharding import Mesh, PartitionSpec as P


F32 = jnp.float32
BF16 = jnp.bfloat16
MESH = pl.DeviceIdType.MESH
VMEM = pl.BlockSpec(memory_space=pltpu.VMEM)


def ring(at, step):
    return lax.rem(at + (step + 4), 4)


def enter(peers):
    barrier = pltpu.get_barrier_semaphore()
    for peer in peers:
        pl.semaphore_signal(barrier, inc=1, device_id=peer, device_id_type=MESH)
    pl.semaphore_wait(barrier, len(peers))


def send(src, dst, send_sems, recv_sems, index, peer):
    copy = pltpu.make_async_remote_copy(src_ref=src, dst_ref=dst, send_sem=send_sems.at[index],
                                        recv_sem=recv_sems.at[index], device_id=peer, device_id_type=MESH)
    copy.start()
    return copy


def line_peers():
    z, dp = lax.axis_index('z'), lax.axis_index('dp')
    up, down = {'z': ring(z, 1)}, {'z': ring(z, -1)}
    return z, dp, up, down, {'dp': 1 - dp}


N_AG = 9


def line_gather(src, dst, send_sems, recv_sems, base):
    for _ in line_gather_steps(src, dst, send_sems, recv_sems, base):
        pass


def line_gather_steps(src, dst, send_sems, recv_sems, base):
    z, dp, up, down, mate = line_peers()
    rows = src.shape[0]
    half = rows // 2
    me = z * 2 + dp
    below, above, far = [ring(z, step) * 2 + dp for step in (-1, 1, 2)]
    lo, hi = pl.ds(0, half), pl.ds(half, half)
    go = functools.partial(send, send_sems=send_sems, recv_sems=recv_sems)
    to_up = go(src, dst.at[me], index=base, peer=up)
    to_down = go(src, dst.at[me], index=base + 1, peer=down)
    to_mate = go(src, dst.at[me], index=base + 2, peer=mate)
    dst[me] = src[...]
    yield
    to_up.wait_recv()
    relay_up = go(dst.at[below, lo], dst.at[below, lo], index=base + 3, peer=up)
    mate_below = go(dst.at[below], dst.at[below], index=base + 5, peer=mate)
    to_down.wait_recv()
    relay_down = go(dst.at[above, hi], dst.at[above, hi], index=base + 4, peer=down)
    mate_above = go(dst.at[above], dst.at[above], index=base + 6, peer=mate)
    yield
    relay_up.wait_recv()
    mate_lo = go(dst.at[far, lo], dst.at[far, lo], index=base + 7, peer=mate)
    relay_down.wait_recv()
    mate_hi = go(dst.at[far, hi], dst.at[far, hi], index=base + 8, peer=mate)
    for copy in (to_mate, mate_below, mate_above, mate_lo, mate_hi):
        copy.wait_recv()
    for copy in (to_up, to_down, to_mate, relay_up, relay_down, mate_below, mate_above, mate_lo, mate_hi):
        copy.wait_send()


N_RS = 10


def line_reduce_steps(part, bufs, send_sems, recv_sems, base):
    d_part, sums, relay_lo, relay_hi, in_lo, in_hi = bufs
    z, dp, up, down, mate = line_peers()
    half = part.shape[1] // 2
    lo, hi = pl.ds(0, half), pl.ds(half, half)
    order = [ring(z, step) for step in (2, 1, -1, 0)]
    go = functools.partial(send, send_sems=send_sems, recv_sems=recv_sems)
    swaps = [go(part.at[zk * 2 + 1 - dp], d_part.at[k], index=base + k, peer=mate) for k, zk in enumerate(order)]
    yield
    swaps[0].wait_recv()
    sums[0] = part[order[0] * 2 + dp] + d_part[0]
    far_up = go(sums.at[0, lo], relay_lo, index=base + 4, peer=up)
    far_down = go(sums.at[0, hi], relay_hi, index=base + 5, peer=down)
    swaps[1].wait_recv()
    sums[1] = part[order[1] * 2 + dp] + d_part[1]
    up_hi = go(sums.at[1, hi], in_lo.at[hi], index=base + 6, peer=up)
    swaps[2].wait_recv()
    sums[2] = part[order[2] * 2 + dp] + d_part[2]
    down_lo = go(sums.at[2, lo], in_hi.at[lo], index=base + 7, peer=down)
    swaps[3].wait_recv()
    sums[3] = part[order[3] * 2 + dp] + d_part[3]
    far_up.wait_recv()
    sums[1, lo] = sums[1, lo] + relay_lo[...]
    up_lo = go(sums.at[1, lo], in_lo.at[lo], index=base + 8, peer=up)
    far_down.wait_recv()
    sums[2, hi] = sums[2, hi] + relay_hi[...]
    down_hi = go(sums.at[2, hi], in_hi.at[hi], index=base + 9, peer=down)
    yield
    for copy in (up_hi, down_lo, up_lo, down_hi):
        copy.wait_recv()
    for copy in swaps + [far_up, far_down, up_hi, down_lo, up_lo, down_hi]:
        copy.wait_send()
    yield sums[3] + in_lo[...] + in_hi[...]


def line_reduce(part, bufs, send_sems, recv_sems, base):
    for total in line_reduce_steps(part, bufs, send_sems, recv_sems, base):
        pass
    return total


def reduce_scratch(tok, width):
    return [pltpu.VMEM((4, tok, width), F32), pltpu.VMEM((4, tok, width), F32),
            pltpu.VMEM((tok // 2, width), F32), pltpu.VMEM((tok // 2, width), F32),
            pltpu.VMEM((tok, width), F32), pltpu.VMEM((tok, width), F32)]


def params(collective_id):
    return pltpu.CompilerParams(collective_id=collective_id, has_side_effects=True,
                                vmem_limit_bytes=60 * 1024 * 1024)


def pass_kernel(transpose, want_all, part, base, w_mix, y_ref, next_ref, *rest):
    if want_all:
        all_ref, rest = rest[0], rest[1:]
    bufs, (send_sems, recv_sems) = rest[:-2], rest[-2:]
    _, _, up, down, mate = line_peers()
    enter((up, down, mate))
    total = line_reduce(part, bufs, send_sems, recv_sems, 0)
    y_val = (base[...].astype(F32) + total).astype(BF16)
    y_ref[...] = y_val
    contract = (((1,), (1 if transpose else 0,)), ((), ()))
    mixed = lax.dot_general(y_val, w_mix[...], contract, preferred_element_type=F32)
    next_ref[...] = (y_val.astype(F32) + mixed).astype(BF16)
    if want_all:
        line_gather(next_ref, all_ref, send_sems, recv_sems, N_RS)


def pass_line(part, base, w_mix, transpose, want_all, collective_id):
    _, tok, width = part.shape
    block = jax.ShapeDtypeStruct((tok, width), BF16)
    outs = [block, block] + ([jax.ShapeDtypeStruct((8, tok, width), BF16)] if want_all else [])
    n_sem = N_RS + (N_AG if want_all else 0)
    return pl.pallas_call(
        functools.partial(pass_kernel, transpose, want_all), name='pass_line',
        out_shape=outs, in_specs=[VMEM] * 3, out_specs=[VMEM] * len(outs),
        scratch_shapes=reduce_scratch(tok, width) + [pltpu.SemaphoreType.DMA((n_sem,)),
                                                     pltpu.SemaphoreType.DMA((n_sem,))],
        compiler_params=params(collective_id))(part, base, w_mix)


def mix_peers():
    at = {axis: lax.axis_index(axis) for axis in 'xyz'}
    return at, {axis: [{axis: ring(at[axis], k)} for k in (1, 2, 3)] for axis in 'xyz'}


def mix_steps(grad, out, bufs, send_sems, recv_sems, base):
    dp = lax.axis_index('dp')
    mate = {'dp': 1 - dp}
    at, peers = mix_peers()
    mate_in, quarter_in, block, y_in, y_out, z_in, z_out = bufs
    quarter = grad.shape[1] // 4
    go = functools.partial(send, send_sems=send_sems, recv_sems=recv_sems)
    copies = []
    swap = go(grad.at[1 - dp], mate_in, index=base, peer=mate)
    yield
    swap.wait_recv()
    block[...] = (grad[dp].astype(F32) + mate_in[...].astype(F32)).astype(BF16)
    mine = pl.ds(pl.multiple_of(at['x'] * quarter, quarter), quarter)
    stage = []
    for k in range(3):
        rows = pl.ds(pl.multiple_of(ring(at['x'], k + 1) * quarter, quarter), quarter)
        stage.append(go(block.at[rows], quarter_in.at[k], index=base + 1 + k, peer=peers['x'][k]))
    copies += [swap] + stage
    yield
    total = block[mine].astype(F32)
    for k in range(3):
        stage[k].wait_recv()
        total = total + quarter_in[k].astype(F32)
    for axis, buf_in, buf_out, first in (('y', y_in, y_out, base + 4), ('z', z_in, z_out, base + 7)):
        buf_out[...] = total.astype(BF16)
        stage = [go(buf_out, buf_in.at[k], index=first + k, peer=peers[axis][k]) for k in range(3)]
        copies += stage
        terms = [buf_out[...].astype(F32)]
        for k in range(3):
            stage[k].wait_recv()
            terms.append(buf_in[k].astype(F32))
        here = at[axis]
        total = None
        for coord in range(4):
            term = jnp.zeros_like(terms[0])
            for k in range(4):
                source = ring(here, -k)
                term = jnp.where(source == coord, terms[k], term)
            total = term if total is None else total + term
    final = total.astype(BF16)
    out[dp, mine] = final
    stage = [go(out.at[dp, mine], out.at[dp, mine], index=base + 10 + k, peer=peers['x'][k]) for k in range(3)]
    copies += stage
    for k in range(3):
        stage[k].wait_recv()
    swap = go(out.at[dp], out.at[dp], index=base + 13, peer=mate)
    swap.wait_recv()
    copies.append(swap)
    for copy in copies:
        copy.wait_send()
    yield


N_MIX = 14


def close_kernel(part_v, base_v, w_mix, x_in, mix_top, part_y, base_y, dx_ref, y_ref, mix_ref, *scratch):
    bufs_v, bufs_y, bufs_m = scratch[:6], scratch[6:12], scratch[12:19]
    grad, send_sems, recv_sems = scratch[19:]
    _, _, _, _, mate = line_peers()
    _, peers = mix_peers()
    enter(peers['x'] + peers['y'] + peers['z'] + [mate])
    steps_v = line_reduce_steps(part_v, bufs_v, send_sems, recv_sems, 0)
    steps_y = line_reduce_steps(part_y, bufs_y, send_sems, recv_sems, N_RS)
    steps_m = mix_steps(grad, mix_ref, bufs_m, send_sems, recv_sems, 2 * N_RS)
    next(steps_v)
    next(steps_y)
    grad[1] = mix_top[...]
    next(steps_v)
    d_u = (base_v[...].astype(F32) + next(steps_v)).astype(BF16)
    grad[0] = tn(x_in[...], d_u).astype(BF16)
    next(steps_m)
    same = unit(d_u.shape[1])
    dx_ref[...] = nt(same, (d_u.astype(F32) + nt(d_u, w_mix[...])).astype(BF16)).astype(BF16)
    next(steps_m)
    next(steps_y)
    next(steps_m)
    y_ref[...] = nt(same, (base_y[...].astype(F32) + next(steps_y)).astype(BF16)).astype(BF16)


def close_line(part_v, base_v, w_mix, x_in, mix_top, part_y, base_y, collective_id):
    _, tok, width = part_v.shape
    quarter = width // 4
    n_sem = 2 * N_RS + N_MIX
    block = jax.ShapeDtypeStruct((width, tok), BF16)
    return pl.pallas_call(
        close_kernel, name='close_line',
        out_shape=[block, block, jax.ShapeDtypeStruct((2, width, width), BF16)],
        in_specs=[VMEM] * 7, out_specs=[VMEM] * 3,
        scratch_shapes=reduce_scratch(tok, width) * 2
        + [pltpu.VMEM((width, width), BF16), pltpu.VMEM((3, quarter, width), BF16), pltpu.VMEM((width, width), BF16)]
        + [pltpu.VMEM((3, quarter, width), BF16), pltpu.VMEM((quarter, width), BF16)] * 2
        + [pltpu.VMEM((2, width, width), BF16), pltpu.SemaphoreType.DMA((n_sem,)), pltpu.SemaphoreType.DMA((n_sem,))],
        compiler_params=params(collective_id))(part_v, base_v, w_mix, x_in, mix_top, part_y, base_y)


N_PLANE = 40
WAYS = (1, -1)
HALVES = (0, 1)


def plane_gather_steps(src, dst, send_sems, recv_sems, base):
    at = {axis: lax.axis_index(axis) for axis in 'xy'}
    rows = src.shape[2] // 2
    part = (pl.ds(0, rows), pl.ds(rows, rows))
    go = functools.partial(send, send_sems=send_sems, recv_sems=recv_sems)
    copies = []

    def block(half, i, j):
        dx, dy = (i, j) if half == 0 else (j, i)
        return ring(at['y'], dy) * 4 + ring(at['x'], dx)

    def peer(half, stage, step):
        axis = 'xy'[stage] if half == 0 else 'yx'[stage]
        return {axis: ring(at[axis], step)}

    counter = [base]

    def launch(half, stage, step, i, j, rows_of=None, own=False):
        b = block(half, i, j)
        to = dst.at[b, :, half] if rows_of is None else dst.at[b, :, half, part[rows_of]]
        copy = go(src.at[:, half] if own else to, to, index=counter[0], peer=peer(half, stage, step))
        counter[0] += 1
        copies.append(copy)
        return copy

    first, second, relay1, relay2 = {}, {}, {}, {}
    for half in HALVES:
        for step in WAYS:
            first[half, step] = launch(half, 0, step, 0, 0, own=True)
    for half in HALVES:
        for step in WAYS:
            second[half, 0, step] = launch(half, 1, step, 0, 0, own=True)
    dst[at['y'] * 4 + at['x']] = src[...]
    yield
    for step in WAYS:
        for half in HALVES:
            first[half, step].wait_recv()
            relay1[half, step] = launch(half, 0, step, -step, 0, rows_of=0 if step == 1 else 1)
            for out in WAYS:
                second[half, -step, out] = launch(half, 1, out, -step, 0)
    yield

    def forward(i):
        for step in WAYS:
            for half in HALVES:
                second[half, i, step].wait_recv()
                relay2[half, i, step] = launch(half, 1, step, i, -step, rows_of=0 if step == 1 else 1)

    forward(0)
    for half in HALVES:
        for step in WAYS:
            relay1[half, step].wait_recv()
        for out in WAYS:
            second[half, 2, out] = launch(half, 1, out, 2, 0)
    yield
    forward(-1)
    forward(1)
    forward(2)
    for copy in relay2.values():
        copy.wait_recv()
    for copy in copies:
        copy.wait_send()
    yield


def open_kernel(n_chip, tokens, d_out, w_mix, ids, gates, w_gate, w_up, w_down,
                tok_all, route, w_all, w_top, u_ref,
                tok_src, route_src, w_src, route_all, load_sems, send_sems, recv_sems):
    z, dp, up, down_peer, mate = line_peers()
    at = {axis: lax.axis_index(axis) for axis in 'xy'}
    n_half = n_chip // 2
    own = pl.ds(dp * n_half, n_half)
    loads = []
    for layer, dst in enumerate((w_src, w_top)):
        for k, (src, to) in enumerate(((w_gate, dst.at[0]), (w_up, dst.at[1]), (w_down, dst.at[2]))):
            loads.append(pltpu.make_async_copy(src.at[layer, own], to, load_sems.at[layer, k]))
    for load in loads:
        load.start()
    enter([up, down_peer, mate] + [{axis: ring(at[axis], k)} for axis in 'xy' for k in WAYS])
    for load in loads[:3]:
        load.wait()
    steps_w = plane_gather_steps(w_src, w_all, send_sems, recv_sems, 0)
    steps_r = line_gather_steps(route_src, route_all, send_sems, recv_sems, N_PLANE)
    steps_t = line_gather_steps(tok_src, tok_all, send_sems, recv_sems, N_PLANE + N_AG)
    next(steps_w)
    width, tok = tokens.shape
    columns = []
    for layer in range(route.shape[0]):
        columns += [ids[layer].astype(F32), *split3(gates[layer])]
    route_src[...] = jnp.concatenate(columns, axis=0).astype(BF16)
    next(steps_r)
    same = unit(width)
    u = (tn(tokens[...], same) + tn(tokens[...], w_mix[0])).astype(BF16)
    u_ref[...] = u
    tok_src[:tok] = u
    tok_src[tok:] = tn(d_out[...], same).astype(BF16)
    next(steps_t)
    for load in loads[3:]:
        load.wait()
    for steps in (steps_r, steps_w, steps_t):
        next(steps)
    next(steps_w)
    for steps in (steps_r, steps_t):
        for _ in steps:
            pass
    n_layers, _, _, n_mine, n_tok = route.shape
    loc = lax.broadcasted_iota(jnp.int32, (n_mine, n_tok), 0)
    mine = ((z * 16 + loc // n_half) * n_chip + dp * n_half + lax.rem(loc, n_half)).astype(F32)
    row = lax.broadcasted_iota(jnp.int32, (n_tok, n_tok), 0)
    col = lax.broadcasted_iota(jnp.int32, (n_tok, n_tok), 1)
    before = jnp.where(row < col, 1.0, 0.0).astype(BF16)
    top_k = route_src.shape[0] // (4 * n_layers)
    for layer in range(n_layers):
        for s in range(8):
            rows = route_all[s, layer * 4 * top_k:(layer + 1) * 4 * top_k, :].astype(F32)
            used = jnp.zeros((n_mine, n_tok), F32)
            gates = [jnp.zeros((n_mine, n_tok), F32) for _ in range(3)]
            for j in range(top_k):
                hit = jnp.broadcast_to(rows[j:j + 1], mine.shape) == mine
                used = jnp.where(hit, 1.0, used)
                for k in range(3):
                    val = rows[(k + 1) * top_k + j:(k + 1) * top_k + j + 1]
                    gates[k] = jnp.where(hit, jnp.broadcast_to(val, mine.shape), gates[k])
            pos = nn(used.astype(BF16), before)
            route[layer, 0, s] = jnp.where(used > 0.5, pos, -1.0)
            for k in range(3):
                route[layer, 1 + k, s] = gates[k]
    for _ in steps_w:
        pass


def open_line(tokens, d_out, w_mix, ids, gates, w_gate, w_up, w_down, collective_id):
    width, tok = tokens.shape
    n_layers, n_chip, _, ff = w_gate.shape
    n_half = n_chip // 2
    n_rows = 4 * n_layers * ids.shape[1]
    n_sem = N_PLANE + 2 * N_AG
    own = (3, n_half, width, ff)
    anywhere = pl.BlockSpec(memory_space=pl.ANY)
    return pl.pallas_call(
        functools.partial(open_kernel, n_chip), name='open_line',
        out_shape=[jax.ShapeDtypeStruct((8, 2 * tok, width), BF16),
                   jax.ShapeDtypeStruct((n_layers, 4, 8, 16 * n_half, tok), F32),
                   jax.ShapeDtypeStruct((16,) + own, BF16), jax.ShapeDtypeStruct(own, BF16),
                   jax.ShapeDtypeStruct((tok, width), BF16)],
        in_specs=[VMEM] * 5 + [anywhere] * 3, out_specs=[VMEM] * 5,
        scratch_shapes=[pltpu.VMEM((2 * tok, width), BF16), pltpu.VMEM((n_rows, tok), BF16), pltpu.VMEM(own, BF16),
                        pltpu.VMEM((8, n_rows, tok), BF16),
                        pltpu.SemaphoreType.DMA((n_layers, 3)),
                        pltpu.SemaphoreType.DMA((n_sem,)), pltpu.SemaphoreType.DMA((n_sem,))],
        compiler_params=params(collective_id))(tokens, d_out, w_mix, ids, gates, w_gate, w_up, w_down)


def silu_parts(pre_gate):
    sig_val = jax.nn.sigmoid(pre_gate)
    return pre_gate * sig_val, sig_val * (1.0 + pre_gate * (1.0 - sig_val))


def split3(val):
    hi = val.astype(BF16).astype(F32)
    rest = val - hi
    mid = rest.astype(BF16).astype(F32)
    return hi, mid, rest - mid


def dot(spec, a, b):
    return jnp.einsum(spec, a, b, preferred_element_type=F32)


CHUNK = 8
TOP_CHUNK = 4
SLOT = 24
ROWS = 8 * SLOT


def one_hot(pos, source, values=None):
    n_experts, n_tok = pos.shape[1:]
    slots = lax.broadcasted_iota(jnp.int32, (SLOT, n_tok), 0).astype(F32)
    blocks = []
    for e in range(n_experts):
        mask = jnp.broadcast_to(pos[source, e:e + 1, :], slots.shape) == slots
        val = 1.0 if values is None else jnp.broadcast_to(values[e:e + 1], slots.shape)
        blocks.append(jnp.where(mask, val, 0.0))
    return jnp.concatenate(blocks, axis=0)


def unit(size):
    row = lax.broadcasted_iota(jnp.int32, (size, size), 0)
    col = lax.broadcasted_iota(jnp.int32, (size, size), 1)
    return jnp.where(row == col, 1.0, 0.0).astype(BF16)


def nn(a, b):
    return lax.dot_general(a, b, (((1,), (0,)), ((), ())), preferred_element_type=F32)


def nt(a, b):
    return lax.dot_general(a, b, (((1,), (1,)), ((), ())), preferred_element_type=F32)


def tn(a, b):
    return lax.dot_general(a, b, (((0,), (0,)), ((), ())), preferred_element_type=F32)


def select_rows(rows_of, out):
    for pair in range(4):
        both = [rows_of(2 * pair), rows_of(2 * pair + 1)]
        for e in range(CHUNK):
            val = jnp.concatenate([rows[e * SLOT:(e + 1) * SLOT] for rows in both], axis=0)
            out[e, pair * 2 * SLOT:(pair + 1) * 2 * SLOT, :] = val.astype(BF16)


def select_tokens(pos, u_all, recv):
    select_rows(lambda s: nn(one_hot(pos, s).astype(BF16), u_all[s]), recv)


def select_grads(pos, hi, mid, lo, dy_all, grad_in):
    def rows_of(s):
        gate_slot = jnp.sum(one_hot(pos, s, (hi[s] + mid[s]) + lo[s]), axis=1, keepdims=True)
        return gate_slot * nn(one_hot(pos, s).astype(BF16), dy_all[s])

    select_rows(rows_of, grad_in)


def hidden_of(rows, w_in, e):
    both = nn(rows, jnp.concatenate([w_in[e // 2, 0, e % 2], w_in[e // 2, 1, e % 2]], axis=1))
    ff = both.shape[1] // 2
    a, b = both[:, :ff], both[:, ff:]
    act, _ = silu_parts(a)
    return a, b, (act * b).astype(BF16)


def expert_grads(c, rows, a, b, h, w_down, e, pack, d_gate, d_up):
    d_hidden = nn(c, w_down)
    act, slope = silu_parts(a)
    da = (d_hidden * b * slope).astype(BF16)
    db = (d_hidden * act).astype(BF16)
    d_gate[e] = da
    d_up[e] = db
    both = tn(rows, jnp.concatenate([da, db], axis=1)).astype(BF16)
    ff = both.shape[1] // 2
    pack[e // 2, 0, e % 2] = both[:, :ff]
    pack[e // 2, 1, e % 2] = both[:, ff:]
    pack[e // 2, 2, e % 2] = tn(c, h).astype(BF16)


def forward_kernel(pos, u_all, w_in, recv, pre_gate, pre_up, hidden):
    select_tokens(pos, u_all, recv)
    for e in range(CHUNK):
        pre_gate[e], pre_up[e], hidden[e] = hidden_of(recv[e], w_in, e)


def backward_kernel(pos, hi, mid, lo, dy_all, w_out, recv, pre_gate, pre_up, hidden, pack, d_gate, d_up, grad_in):
    select_grads(pos, hi, mid, lo, dy_all, grad_in)
    for e in range(CHUNK):
        expert_grads(grad_in[e], recv[e], pre_gate[e], pre_up[e], hidden[e], w_out[e // 2, 0, e % 2], e,
                     pack, d_gate, d_up)


def select_kernel(pos, hi, mid, lo, u_all, dy_all, recv, grad_in):
    select_tokens(pos, u_all, recv)
    select_grads(pos, hi, mid, lo, dy_all, grad_in)


def top_kernel(recv, grad_in, w_all, pack, d_gate, d_up, hidden):
    for e in range(TOP_CHUNK):
        rows = recv[e]
        a, b, h = hidden_of(rows, w_all, e)
        hidden[e] = h
        expert_grads(grad_in[e], rows, a, b, h, w_all[e // 2, 2, e % 2], e, pack, d_gate, d_up)


def combine_kernel(n_left, pos, hi, mid, lo, *refs):
    lefts, w_out, part, rows = refs[:n_left], refs[n_left], refs[n_left + 1], refs[n_left + 2]
    step = pl.program_id(0)
    for e in range(CHUNK):
        left = jnp.concatenate([ref[e] for ref in lefts], axis=1)
        right = jnp.concatenate([w_out[e // 2, k, e % 2] for k in range(n_left)], axis=1)
        rows[step * CHUNK + e] = nt(left, right).astype(BF16).astype(F32)

    @pl.when(step == pl.num_programs(0) - 1)
    def _():
        def source(s, carry):
            slots = pl.ds(pl.multiple_of(s * SLOT, 8), SLOT)
            mine = jnp.concatenate([rows[e, slots, :] for e in range(rows.shape[0])], axis=0).astype(BF16)
            val = tn(one_hot(pos, s, lo[s]).astype(BF16), mine)
            val = val + tn(one_hot(pos, s, mid[s]).astype(BF16), mine)
            part[s] = val + tn(one_hot(pos, s, hi[s]).astype(BF16), mine)
            return carry

        lax.fori_loop(0, 8, source, 0)


def route_specs(route, layer, kinds, n_experts=CHUNK):
    pick = (lambda i: i) if n_experts == CHUNK else (lambda i: 0)
    return [pl.BlockSpec((None, None, 8, n_experts, route.shape[4]), lambda i, k=k: (layer, k, 0, pick(i), 0))
            for k in kinds]


def token_spec(tok_all, n_tok, part):
    return pl.BlockSpec((8, n_tok, tok_all.shape[2]), lambda i: (0, part, 0))


def per_expert(last, chunk=CHUNK):
    return pl.BlockSpec((chunk, ROWS, last), lambda i: (i, 0, 0))


def weight_spec(weights, kinds, first, chunk=CHUNK):
    return pl.BlockSpec((chunk // 2, kinds, 2) + weights.shape[3:], lambda i: (i, first // kinds, 0, 0, 0))


def local_call(kernel, n_mine, outs, in_specs, out_specs, scratch=(), chunk=CHUNK):
    return pl.pallas_call(
        kernel, grid=(n_mine // chunk,), out_shape=outs, in_specs=in_specs, out_specs=out_specs,
        scratch_shapes=list(scratch), compiler_params=pltpu.CompilerParams(vmem_limit_bytes=60 * 1024 * 1024))


def per_slot(n_mine, last, dtype):
    return jax.ShapeDtypeStruct((n_mine, ROWS, last), dtype)


def expert_forward(route, layer, u_all, weights):
    n_mine, n_tok = route.shape[3:]
    width, ff = weights.shape[3:]
    return local_call(
        forward_kernel, n_mine,
        [per_slot(n_mine, width, BF16), per_slot(n_mine, ff, F32), per_slot(n_mine, ff, F32), per_slot(n_mine, ff, BF16)],
        route_specs(route, layer, (0,)) + [token_spec(u_all, n_tok, 0), weight_spec(weights, 2, 0)],
        [per_expert(width), per_expert(ff), per_expert(ff), per_expert(ff)])(route, u_all, weights)


def expert_backward(route, layer, dy_all, weights, recv, pre_gate, pre_up, hidden):
    n_mine, n_tok = route.shape[3:]
    width, ff = weights.shape[3:]
    return local_call(
        backward_kernel, n_mine,
        [jax.ShapeDtypeStruct(weights.shape, BF16), per_slot(n_mine, ff, BF16), per_slot(n_mine, ff, BF16)],
        route_specs(route, layer, range(4)) + [token_spec(dy_all, n_tok, 0), weight_spec(weights, 1, 2),
                                                   per_expert(width), per_expert(ff), per_expert(ff), per_expert(ff)],
        [weight_spec(weights, 3, 0), per_expert(ff), per_expert(ff)],
        [pltpu.VMEM((CHUNK, ROWS, width), BF16)])(*[route] * 4, dy_all, weights, recv, pre_gate, pre_up, hidden)


def expert_select(route, layer, u_all, dy_all, dy_part):
    n_mine, n_tok = route.shape[3:]
    width = u_all.shape[2]
    return local_call(
        select_kernel, n_mine, [per_slot(n_mine, width, BF16)] * 2,
        route_specs(route, layer, range(4)) + [token_spec(u_all, n_tok, 0), token_spec(dy_all, n_tok, dy_part)],
        [per_expert(width)] * 2)(*[route] * 4, u_all, dy_all)


def expert_top(recv, grad_in, weights):
    n_mine = recv.shape[0]
    width, ff = weights.shape[3:]
    return local_call(
        top_kernel, n_mine,
        [jax.ShapeDtypeStruct(weights.shape, BF16)] + [per_slot(n_mine, ff, BF16)] * 3,
        [per_expert(width, TOP_CHUNK)] * 2 + [weight_spec(weights, 3, 0, TOP_CHUNK)],
        [weight_spec(weights, 3, 0, TOP_CHUNK)] + [per_expert(ff, TOP_CHUNK)] * 3, chunk=TOP_CHUNK)(
            recv, grad_in, weights)


def expert_combine(route, layer, lefts, weights, which):
    n_mine, n_tok = route.shape[3:]
    width, ff = weights.shape[3:]
    return local_call(
        functools.partial(combine_kernel, len(lefts)), n_mine,
        jax.ShapeDtypeStruct((8, n_tok, width), F32),
        route_specs(route, layer, range(4), n_mine) + [per_expert(ff)] * len(lefts)
        + [weight_spec(weights, len(lefts), which)],
        pl.BlockSpec((8, n_tok, width), lambda i: (0, 0, 0)),
        [pltpu.VMEM((n_mine, ROWS, width), F32)])(*[route] * 4, *lefts, weights)


def solution(mesh):
    m4 = Mesh(mesh.devices.reshape(4, 4, 4, 2), ('z', 'y', 'x', 'dp'))
    ep = ('z', 'y', 'x')
    tok_spec = P(('dp',) + ep, None)
    route_spec = P(None, ('dp',) + ep, None)
    whole_spec = P(None, None, None)
    expert_spec = P(None, ep, None, None)

    def device_body(tokens, d_out, expert_ids, gate_vals, w_mix, w_gate, w_up, w_down):
        n_chip = w_gate.shape[1]
        n_half = n_chip // 2
        _, d_model = tokens.shape
        ff = w_gate.shape[3]
        dp = lax.axis_index('dp')

        def scatter_grads(pack):
            part = lax.psum_scatter(pack.reshape(16 * 3 * n_half * d_model, ff), ('y', 'x'),
                                    scatter_dimension=0, tiled=True)
            return part

        def finish_grads(part):
            other = lax.ppermute(part, 'dp', [(0, 1), (1, 0)])
            lo = jnp.where(dp == 0, part, other).reshape(3, n_half, d_model, ff)
            hi = jnp.where(dp == 0, other, part).reshape(3, n_half, d_model, ff)
            both = jnp.concatenate([lo, hi], axis=1)
            return both[0], both[1], jnp.swapaxes(both[2], 1, 2)

        tok_all, route, w_first, own_top, u_act = open_line(
            tokens.T, d_out.T, w_mix, jnp.swapaxes(expert_ids, 1, 2), jnp.swapaxes(gate_vals, 1, 2),
            w_gate, w_up, jnp.swapaxes(w_down, 2, 3), 1)
        w_top = lax.all_gather(own_top.reshape(3 * n_half * d_model, ff), ('y', 'x'), axis=0, tiled=False)
        w_top = w_top.reshape(16, 3, n_half, d_model, ff)

        low = expert_forward(route, 0, tok_all, w_first)
        part = expert_combine(route, 0, low[3:], w_first, 2)
        y_low, u_top, u_all = pass_line(part, u_act, w_mix[1], False, True, 2)

        recv, grad_in = expert_select(route, 1, u_all, tok_all, 1)
        w_top, recv = lax.optimization_barrier((w_top, recv))
        pack, d_gate, d_up, hidden = expert_top(recv, grad_in, w_top)
        grad_top = scatter_grads(pack)
        part = expert_combine(route, 1, (d_gate, d_up), w_top, 0)
        d_u, d_y, dy_all = pass_line(part, d_out, w_mix[1], True, True, 3)
        mix_top = dot('td,te->de', y_low, d_u).astype(BF16)

        pack, d_gate, d_up = expert_backward(route, 0, dy_all, w_first, *low)
        grad_low = scatter_grads(pack)
        part_v = expert_combine(route, 0, (d_gate, d_up), w_first, 0)
        hidden, part_v = lax.optimization_barrier((hidden, part_v))
        part_y = expert_combine(route, 1, (hidden,), w_top, 2)
        d_tokens, layer_out, mix_out = close_line(part_v, d_y, w_mix[0], tokens, mix_top, part_y, u_top, 4)
        grad_top, d_tokens = lax.optimization_barrier((grad_top, d_tokens))
        grads = [finish_grads(grad_low), finish_grads(grad_top)]
        return (layer_out.T, d_tokens.T, mix_out) + tuple(jnp.stack([g[k] for g in grads]) for k in range(3))

    return jax.shard_map(device_body, mesh=m4,
                         in_specs=(tok_spec, tok_spec, route_spec, route_spec, whole_spec,
                                   expert_spec, expert_spec, expert_spec),
                         out_specs=(tok_spec, tok_spec, whole_spec, expert_spec, expert_spec, expert_spec),
                         check_vma=False)
```
